32 devices in a mesh: rows: 8 (over z, x), leaf: 4 (over y, core).
Axes of the slice: x: 2, y: 2, z: 4, core: 2. Of those that a mesh axis runs over, the one named last changes fastest.
Arguments:
- right_sides: float32 [65536, 128], P(('rows', 'leaf')), may hold values from -30 to 30
- near_blocks: bfloat16 [2, 128, 512, 512], P(None, ('rows', 'leaf')), may hold values from -1 to 2.4
- leaf_bases: bfloat16 [2, 128, 2, 512, 128], P(None, ('rows', 'leaf')), may hold values from -1.5 to 1.5
- local_factors: bfloat16 [2, 224, 3, 128, 128], P(None, ('rows', 'leaf')), may hold values from -1.7 to 1.7
- upper_factors: bfloat16 [2, 32, 3, 3, 128, 128], P(None, ('rows', 'leaf')), may hold values from -1.7 to 1.7, as said below
- top_couplings: bfloat16 [2, 2, 128, 128], replicated, may hold values from -0.5 to 0.5
Outputs:
- solution: float32 [65536, 128], P(('rows', 'leaf'))
- residual_norms: float32 [3, 128], replicated
The draws below stay inside these ranges and needn't reach their ends.
Inputs may be any that keep to these rules, and one draw needn't show every extreme that they name: upper_factors[s, d, h] is the same for all devices d with the same d // 2 ** (h + 1): the factors of the node h + 1 levels above device d's own node.
All inputs are finite; a program needn't handle non-finite values.
Results may differ from the reference program's by a relative error of at most 0.00095.
Values sent between devices are 32-bit elements; how exact they have to be, the bound alone decides.
No kernel may reach another device: no remote copies, remote signals or barrier semaphores. Data moves between devices by JAX's collectives and lax.ppermute only.
A program may use at most 128 MiB of HBM per device.

```python
import math
import jax
import jax.numpy as jnp
from jax import lax

LEAF = 512
RANK = 128
RHS = 128
LEAF_DEV = 4
STEPS = 3
UPPER = 3
NLEAVES = 128
ORDER = 65536
N_ROWS = 8
N_LEAF = 4


def clipped(key_value, shape):
    return jnp.clip(jax.random.normal(key_value, shape, jnp.float32), -6.0, 6.0)


def node_factors(key_value, node_count):
    keys = jax.random.split(key_value, 6)
    shape = (node_count, RANK, RANK)
    spread = RANK ** (-0.5)
    identity_matrix = jnp.eye(RANK, dtype=jnp.float32)
    up_transfer = (identity_matrix + 0.3 * spread * clipped(keys[0], shape)) * 0.7071
    down_transfer = (identity_matrix + 0.3 * spread * clipped(keys[1], shape)) * 0.96
    coupling = 0.1 * spread * clipped(keys[2], shape)
    operator_part = jnp.stack([up_transfer, down_transfer, coupling], axis=1)
    inverse_part = jnp.stack([up_transfer + 0.05 * spread * clipped(keys[3], shape), down_transfer + 0.05 * spread * clipped(keys[4], shape), 0.02 * spread * clipped(keys[5], shape) - coupling], axis=1)
    return (operator_part, inverse_part)


def draw_right_sides(key, part):
    first_key = jax.random.fold_in(jax.random.fold_in(key, 606), 0)
    growth = jnp.exp(math.log(3.0) * jnp.arange(ORDER, dtype=jnp.float32) / ORDER)
    return clipped(first_key, (ORDER, RHS)) * growth[:, None]


def draw_near_blocks(key, part):
    keys = jax.random.split(jax.random.fold_in(key, 404), 3)
    diagonal_gain = jax.random.uniform(keys[0], (NLEAVES, LEAF), jnp.float32, 0.8, 1.25)
    coupling = clipped(keys[1], (NLEAVES, LEAF, LEAF)) * (0.2 * LEAF ** (-0.5))
    noise_term = clipped(keys[2], (NLEAVES, LEAF, LEAF)) * (0.45 * LEAF ** (-0.5))
    identity_matrix = jnp.eye(LEAF, dtype=jnp.float32)
    operator_block = identity_matrix * diagonal_gain[:, :, None] + coupling
    inverse_gain = 1.0 / diagonal_gain
    inverse_block = identity_matrix * inverse_gain[:, :, None] - inverse_gain[:, :, None] * coupling * inverse_gain[:, None, :] + noise_term
    return jnp.stack([operator_block, inverse_block]).astype(jnp.bfloat16)


def draw_leaf_bases(key, part):
    first_key, second_key = jax.random.split(jax.random.fold_in(key, 505))
    shape = (NLEAVES, 2, LEAF, RANK)
    operator_bases = clipped(first_key, shape) * LEAF ** (-0.5)
    inverse_bases = operator_bases + 0.1 * clipped(second_key, shape) * LEAF ** (-0.5)
    return jnp.stack([operator_bases, inverse_bases]).astype(jnp.bfloat16)


def draw_local_factors(key, part):
    operator_part, inverse_part = node_factors(jax.random.fold_in(key, 101), (2 * LEAF_DEV - 1) * N_ROWS * N_LEAF)
    return jnp.stack([operator_part, inverse_part]).astype(jnp.bfloat16)


def draw_upper_factors(key, part):
    operator_levels = []
    inverse_levels = []
    for height in range(1, UPPER + 1):
        node_count = N_ROWS * N_LEAF // 2 ** height
        operator_part, inverse_part = node_factors(jax.random.fold_in(jax.random.fold_in(key, 202), height), node_count)
        operator_levels.append(jnp.repeat(operator_part, 2 ** height, axis=0))
        inverse_levels.append(jnp.repeat(inverse_part, 2 ** height, axis=0))
    return jnp.stack([jnp.stack(operator_levels, axis=1), jnp.stack(inverse_levels, axis=1)]).astype(jnp.bfloat16)


def draw_top_couplings(key, part):
    first_key, second_key = jax.random.split(jax.random.fold_in(key, 303))
    spread = RANK ** (-0.5)
    coupling = 0.1 * spread * clipped(first_key, (2, RANK, RANK))
    inverse_coupling = 0.02 * spread * clipped(second_key, (2, RANK, RANK)) - coupling
    return jnp.stack([coupling, inverse_coupling]).astype(jnp.bfloat16)


def setup_inputs(seed: int = 0) -> dict:
    seeds = jax.random.split(jax.random.key(seed), 7)
    return {
        "right_sides": draw_right_sides(jax.random.fold_in(seeds[6], 71), 0),
        "near_blocks": draw_near_blocks(jax.random.fold_in(seeds[6], 71), 0),
        "leaf_bases": draw_leaf_bases(jax.random.fold_in(seeds[6], 71), 0),
        "local_factors": draw_local_factors(jax.random.fold_in(seeds[6], 71), 0),
        "upper_factors": draw_upper_factors(jax.random.fold_in(seeds[6], 71), 0),
        "top_couplings": draw_top_couplings(jax.random.fold_in(seeds[6], 71), 0),
    }


HIGHEST = lax.Precision.HIGHEST


def split_pair(values):
    upper_half = lax.optimization_barrier(values.astype(jnp.bfloat16))
    lower_half = (values - upper_half.astype(jnp.float32)).astype(jnp.bfloat16)
    return (upper_half, lower_half)


def sibling_of(values):
    shaped = values.reshape((values.shape[0] // 2, 2) + values.shape[1:])
    return shaped[:, ::-1].reshape(values.shape)


def level_tables(local_factors, upper_factors, member):
    per_device = local_factors[member].reshape(N_ROWS * N_LEAF, 2 * LEAF_DEV - 1, 3, RANK, RANK)
    tables = []
    offset = 0
    node_count = LEAF_DEV
    while node_count >= 1:
        factor_block = per_device[:, offset:offset + node_count]
        tables.append(factor_block.reshape(-1, 3, RANK, RANK).astype(jnp.float32))
        offset = offset + node_count
        node_count = node_count // 2
    for height in range(1, UPPER + 1):
        tables.append(upper_factors[member, ::2 ** height, height - 1].astype(jnp.float32))
    return tables


def near_and_coefficient(items):
    square, column_basis, stacked_pieces = items
    near_field = jnp.zeros((square.shape[0], stacked_pieces.shape[2]), jnp.float32)
    coefficient = jnp.zeros((column_basis.shape[1], stacked_pieces.shape[2]), jnp.float32)
    for piece_index in range(stacked_pieces.shape[0]):
        piece_value = stacked_pieces[piece_index]
        near_field = near_field + jnp.dot(square, piece_value, preferred_element_type=jnp.float32)
        coefficient = coefficient + jnp.dot(column_basis.T, piece_value, preferred_element_type=jnp.float32)
    return near_field, coefficient


def far_product(items):
    row_basis, stacked_far = items
    result = jnp.zeros((row_basis.shape[0], stacked_far.shape[2]), jnp.float32)
    for piece_index in range(stacked_far.shape[0]):
        result = result + jnp.dot(row_basis, stacked_far[piece_index], preferred_element_type=jnp.float32)
    return result


def apply_tree(near_set, basis_set, tables, top_pair, pieces, split_far):
    stacked = jnp.stack(pieces, axis=1)
    near_field, coefficient = lax.map(near_and_coefficient, (near_set, basis_set[:, 1], stacked))
    lower_list = []
    for factor_table in tables:
        lower_list.append(coefficient)
        projected = jnp.einsum("nab,nac->nbc", factor_table[:, 0], coefficient, precision=HIGHEST)
        coefficient = projected[0::2] + projected[1::2]
    far_field = jnp.einsum("nab,nbc->nac", top_pair.astype(jnp.float32), sibling_of(coefficient), precision=HIGHEST)
    for factor_table, lower_value in zip(tables[::-1], lower_list[::-1]):
        far_field = jnp.einsum("nab,nbc->nac", factor_table[:, 1], jnp.repeat(far_field, 2, axis=0), precision=HIGHEST) + jnp.einsum("nab,nbc->nac", factor_table[:, 2], sibling_of(lower_value), precision=HIGHEST)
    if split_far:
        far_parts = split_pair(far_field)
    else:
        far_parts = (far_field.astype(jnp.bfloat16),)
    return near_field + lax.map(far_product, (basis_set[:, 0], jnp.stack(far_parts, axis=1)))


def reference(right_sides, near_blocks, leaf_bases, local_factors, upper_factors, top_couplings):
    leaves = right_sides.shape[0] // LEAF
    right_side = right_sides.reshape(leaves, LEAF, RHS)
    tables_operator = level_tables(local_factors, upper_factors, 0)
    tables_inverse = level_tables(local_factors, upper_factors, 1)

    def operator(values):
        return apply_tree(near_blocks[0], leaf_bases[0], tables_operator, top_couplings[0], split_pair(values), True)

    def inverse(values):
        return apply_tree(near_blocks[1], leaf_bases[1], tables_inverse, top_couplings[1], (values.astype(jnp.bfloat16),), False)

    solution = inverse(right_side)
    norm_list = []
    for refine_step in range(STEPS):
        residual = right_side - operator(solution)
        norm_list.append(jnp.sum(residual * residual, axis=(0, 1)))
        solution = solution + inverse(residual)
    return (solution.reshape(right_sides.shape[0], RHS), jnp.stack(norm_list))
```

```python
import jax
import jax.numpy as jnp
from jax import lax
from jax.sharding import PartitionSpec as P

STEPS = 3
HIGHEST = lax.Precision.HIGHEST


def dot(left, right):
    return jnp.dot(left, right, precision=HIGHEST)


def swapped(value, level, bits_leaf):
    axis, shift = ("leaf", level) if level < bits_leaf else ("rows", level - bits_leaf)
    mask = 2**shift
    pairs = [(source, source ^ mask) for source in range(lax.axis_size(axis))]
    return lax.ppermute(value, axis, pairs)


def split_pair(values):
    upper_half = lax.optimization_barrier(values.astype(jnp.bfloat16))
    lower_half = (values - upper_half.astype(jnp.float32)).astype(jnp.bfloat16)
    return (upper_half, lower_half)


def pieces_of(values, split):
    return split_pair(values) if split else (values.astype(jnp.bfloat16),)


def device_tree(factors, leaf_count):
    levels = []
    offset = 0
    count = leaf_count
    while count >= 1:
        levels.append(factors[offset : offset + count])
        offset += count
        count //= 2
    own = levels[-1][0]
    rank = own.shape[-1]
    identity = jnp.eye(rank, dtype=jnp.float32)
    ups = [[identity] for _ in range(leaf_count)]
    for depth in range(len(levels) - 1):
        for leaf in range(leaf_count):
            ups[leaf].append(dot(ups[leaf][-1], levels[depth][leaf >> depth, 0]))
    down_device = [None] * leaf_count
    inner = [[None] * leaf_count for _ in range(leaf_count)]
    for leaf in range(leaf_count):
        trail = identity
        for depth in range(len(levels) - 1):
            node = leaf >> depth
            table = levels[depth][node]
            coupled = dot(table[2].T, trail)
            for other in range(leaf_count):
                if other >> depth == node ^ 1:
                    inner[other][leaf] = dot(ups[other][depth], coupled)
            trail = dot(table[1].T, trail)
        inner[leaf][leaf] = jnp.zeros_like(identity)
        down_device[leaf] = trail
    up = jnp.stack([chain[-1] for chain in ups])
    down = jnp.stack([dot(own[1].T, trail) for trail in down_device])
    across = jnp.stack([dot(own[2].T, trail) for trail in down_device])
    inner = jnp.stack([jnp.stack(row) for row in inner])
    return up, down, across, inner, own[0]


def body(right_sides, near_blocks, leaf_bases, local_factors, upper_factors, top_couplings):
    bits_leaf = lax.axis_size("leaf").bit_length() - 1
    bits_rows = lax.axis_size("rows").bit_length() - 1
    levels_up = bits_leaf + bits_rows
    leaf_count = near_blocks.shape[1]
    columns = right_sides.shape[1]
    half = columns // 2
    core = lax.axis_index("leaf") % 2
    top_position = lax.axis_index("rows") // 2 ** (bits_rows - 1) % 2
    right_side = right_sides.reshape(leaf_count, -1, columns)

    trees = []
    siblings = []
    gathers = []
    owns = []
    upper = upper_factors[:, 0].astype(jnp.float32)
    local = local_factors.astype(jnp.float32)
    for level in range(1, levels_up - 1):
        both = upper[:, level - 1, 0].reshape(-1, upper.shape[-1])
        siblings.append(swapped(both, level, bits_leaf).reshape(2, -1, upper.shape[-1]))
    for member in range(2):
        trees.append(device_tree(local[member], leaf_count))
        top = lax.dynamic_index_in_dim(top_couplings[member], top_position, 0, keepdims=False)
        terms = []
        trail = None
        for level in range(1, levels_up):
            coupling = (
                top.astype(jnp.float32) if level == levels_up - 1 else upper[member, level - 1, 2]
            )
            terms.append(coupling.T if trail is None else dot(coupling.T, trail))
            if level < levels_up - 1:
                step = upper[member, level - 1, 1].T
                trail = step if trail is None else dot(step, trail)
        gathers.append(terms)
        owns.append([upper[member, level - 1, 0] for level in range(1, levels_up - 1)])

    def lift(member, coefficient):
        up, _, _, _, transfer = trees[member]
        device = jnp.einsum("lnr,lrq->nq", coefficient, up, precision=HIGHEST)
        return device, dot(device, transfer)

    def coefficients(member, pieces):
        total = None
        for piece in pieces:
            term = jnp.einsum(
                "lin,lir->lnr", piece, leaf_bases[member, :, 1], preferred_element_type=jnp.float32
            )
            total = term if total is None else total + term
        return total

    def near(member, pieces):
        total = None
        for piece in pieces:
            term = jnp.einsum(
                "lij,ljn->lin", near_blocks[member], piece, preferred_element_type=jnp.float32
            )
            total = term if total is None else total + term
        return total

    def expand(member, far):
        total = None
        for piece in pieces_of(far, member == 0):
            term = jnp.einsum(
                "lir,lnr->lin", leaf_bases[member, :, 0], piece, preferred_element_type=jnp.float32
            )
            total = term if total is None else total + term
        return total

    def mine(value):
        return lax.dynamic_slice_in_dim(value, core * half, half, 0)

    def chip_sum(device, lifted):
        received = swapped(jnp.concatenate([device, lifted]), 0, bits_leaf)
        return received[:columns], mine(lifted + received[columns:])

    leaf_feed, chip_feed, sibling_feed = [], [], []
    stacked = []
    for member in range(2):
        other = 1 - member
        sign = 1.0 if member == 1 else -1.0
        feed = jnp.einsum(
            "lir,liq->lrq",
            leaf_bases[member, :, 0],
            leaf_bases[other, :, 1],
            preferred_element_type=jnp.float32,
        )
        feed = sign * jnp.einsum("lpr,lrq->lpq", trees[member][1], feed, precision=HIGHEST)
        leaf_feed.append(feed)
        device = jnp.einsum("lpr,lrq->pq", feed, trees[other][0], precision=HIGHEST)
        stacked.append(device)
        stacked.append(dot(device, trees[other][4]))
    stacked = jnp.stack(stacked)
    received = swapped(stacked.reshape(-1, stacked.shape[-1]), 0, bits_leaf).reshape(stacked.shape)
    for member in range(2):
        sibling_feed.append(received[2 * member])
        chip_feed.append(stacked[2 * member + 1] + received[2 * member + 1])
    gather_feed = [[dot(term, chip_feed[member]) for term in gathers[member]] for member in range(2)]

    applies = 2 * STEPS + 1
    solution = jnp.zeros_like(right_side)
    member = 1
    pieces = pieces_of(right_side, False)
    coefficient = coefficients(member, pieces)
    sibling, chip = chip_sum(*lift(member, coefficient))
    norms = []
    for index in range(applies):
        last = index == applies - 1
        other = 1 - member
        level_coefficient = chip
        far = None
        feed = None
        arrived = []
        for level in range(1, levels_up):
            value = swapped(level_coefficient, level, bits_leaf)
            arrived.append(value)
            if level < levels_up - 1:
                level_coefficient = dot(level_coefficient, owns[member][level - 1]) + dot(
                    value, siblings[level - 1][member]
                )
        _, down, across, inner, _ = trees[member]
        far_local = jnp.einsum("nr,lrq->lnq", sibling, across, precision=HIGHEST)
        far_local = far_local + jnp.einsum("jnr,jlrq->lnq", coefficient, inner, precision=HIGHEST)
        partial = near(member, pieces) + expand(member, far_local)
        partial = solution + partial if member == 1 else right_side - partial
        if not last:
            next_pieces = pieces_of(partial, other == 0)
            next_coefficient = coefficients(other, next_pieces)
            next_sibling, feed = chip_sum(*lift(other, next_coefficient))
        for value, term in zip(arrived, gathers[member]):
            far = dot(value, term) if far is None else far + dot(value, term)
        if not last:
            for value, term in zip(arrived, gather_feed[member]):
                feed = feed + dot(value, term)
            chip = feed
        partner = swapped(far, 0, bits_leaf)
        far = jnp.where(
            core == 0, jnp.concatenate([far, partner]), jnp.concatenate([partner, far])
        )
        sign = 1.0 if member == 1 else -1.0
        far_leaf = jnp.einsum("nr,lrq->lnq", far, down, precision=HIGHEST)
        values = partial + sign * expand(member, far_leaf)
        if member == 1:
            solution = values
        else:
            norms.append(jnp.sum(values * values, axis=(0, 1)))
        if not last:
            coefficient = next_coefficient + jnp.einsum(
                "nr,lrq->lnq", far, leaf_feed[member], precision=HIGHEST
            )
            sibling = next_sibling + dot(far, sibling_feed[member])
            pieces = pieces_of(values, other == 0)
        member = other
    norm_table = jnp.stack(norms)
    for level in range(levels_up):
        norm_table = norm_table + swapped(norm_table, level, bits_leaf)
    return (solution.reshape(-1, columns), norm_table)


def solution(mesh):
    placed = (
        P(("rows", "leaf"), None),
        P(None, ("rows", "leaf"), None, None),
        P(None, ("rows", "leaf"), None, None, None),
        P(None, ("rows", "leaf"), None, None, None),
        P(None, ("rows", "leaf"), None, None, None, None),
        P(),
    )
    return jax.shard_map(
        body,
        mesh=mesh,
        in_specs=placed,
        out_specs=(P(("rows", "leaf"), None), P()),
        check_vma=False,
    )
```

```python
import functools

import jax
import jax.numpy as jnp
from jax import lax
from jax.experimental import pallas as pl
from jax.experimental.pallas import tpu as pltpu
from jax.sharding import PartitionSpec as P

STEPS = 3
BF16 = jnp.bfloat16
F32 = jnp.float32
VMEM_LIMIT = 16 * 2**20


def mm(left, right):
    return jnp.dot(left, right, preferred_element_type=F32)


def pieces(value):
    high = value.astype(BF16)
    return high, (value - high.astype(F32)).astype(BF16)


def left_mul(table, value):
    high, low = pieces(value)
    width = value.shape[1]
    both = mm(table[0], jnp.concatenate([high, low], axis=1))
    return both[:, :width] + both[:, width:] + mm(table[1], high)


def right_mul(value, table):
    high, low = pieces(value)
    rows = value.shape[0]
    both = mm(jnp.concatenate([high, low], axis=0), table[0])
    return both[:rows] + both[rows:] + mm(high, table[1])


def mul(left, right):
    return left_mul(pieces(left), right)


def exact_left(table, value):
    high, low = pieces(value)
    width = value.shape[1]
    both = mm(table, jnp.concatenate([high, low], axis=1))
    return both[:, :width] + both[:, width:]


def exact_right(value, table):
    high, low = pieces(value)
    rows = value.shape[0]
    both = mm(jnp.concatenate([high, low], axis=0), table)
    return both[:rows] + both[rows:]


def put(ref, index, value):
    high, low = pieces(value)
    ref[(0,) + index] = high
    ref[(1,) + index] = low


def call(kernel, outs, args, flops):
    specs = [pl.BlockSpec(memory_space=pltpu.SMEM)]
    specs += [pl.BlockSpec(memory_space=pltpu.VMEM)] * (len(args) - 1)
    return pl.pallas_call(
        kernel,
        out_shape=[jax.ShapeDtypeStruct(shape, dtype) for shape, dtype in outs],
        in_specs=specs,
        out_specs=[pl.BlockSpec(memory_space=pltpu.VMEM)] * len(outs),
        compiler_params=pltpu.CompilerParams(vmem_limit_bytes=VMEM_LIMIT),
        cost_estimate=pl.CostEstimate(flops=flops, bytes_accessed=0, transcendentals=0),
    )(*args)


def level_offsets(leaf_count):
    offsets, count, offset = [], leaf_count, 0
    while count >= 1:
        offsets.append(offset)
        offset += count
        count //= 2
    return offsets


def send_parts(core, device, lifted, send_ref, keep_ref):
    columns = lifted.shape[1]
    half = columns // 2
    turned = lifted.T
    first = core == 0
    keep_ref[...] = jnp.where(first, turned[:half], turned[half:])
    send_ref[: device.shape[0]] = device
    send_ref[device.shape[0] :] = jnp.where(first, turned[half:], turned[:half])


def start_kernel(leaves, core_ref, right_ref, vt_ref, pt_ref, up_ref, coef_ref, send_ref, keep_ref):
    rank = pt_ref.shape[-1]
    offsets = level_offsets(leaves)
    for member in (1, 0):
        for leaf in range(leaves):
            trail = pt_ref[member, leaf].astype(F32)
            for depth in range(1, len(offsets)):
                table = pt_ref[member, offsets[depth] + (leaf >> depth)]
                if depth == len(offsets) - 1:
                    put(up_ref, (member, slice(0, rank), pl.ds(leaf * rank, rank)), trail)
                trail = exact_left(table, trail)
            put(up_ref, (member, slice(rank, 2 * rank), pl.ds(leaf * rank, rank)), trail)
    rows = right_ref.shape[0] // leaves
    for leaf in range(leaves):
        value = right_ref[leaf * rows : (leaf + 1) * rows].astype(BF16)
        coef_ref[leaf * rank : (leaf + 1) * rank] = mm(vt_ref[1, leaf], value)
    lifted = left_mul((up_ref[0, 1], up_ref[1, 1]), coef_ref[...])
    send_parts(core_ref[0], lifted[:rank], lifted[rank:], send_ref, keep_ref)


def stage_table_kernel(core_ref, own_ref, *refs):
    near_ref, far_ref, cross_ref, out_ref = refs
    rank = own_ref.shape[-1]
    for member in range(2):
        here = own_ref[member, 1].astype(BF16)
        there = far_ref[2 + member].astype(BF16)
        lowers = (own_ref[member, 0], near_ref[member], far_ref[member], cross_ref[member])
        for index, (lower, upper) in enumerate(zip(lowers, (here, here, there, there))):
            put(out_ref, (member, pl.ds(index * rank, rank)), mm(lower.astype(BF16), upper))


def local_table_kernel(
    leaves, core_ref, pt_ref, qc_ref, u_ref, vt_ref, up_ref, wide_ref, down_ref, feed_ref, chip_ref
):
    rank = pt_ref.shape[-1]
    offsets = level_offsets(leaves)
    own = offsets[-1]
    for member in range(2):
        other = 1 - member
        sign = 1.0 if member == 1 else -1.0
        total = None
        for leaf in range(leaves):
            rows = pl.ds(leaf * rank, rank)
            trail = None
            for depth in range(len(offsets) - 1):
                node = leaf >> depth
                step = qc_ref[member, offsets[depth] + node, 0]
                coupling = qc_ref[member, offsets[depth] + node, 1]
                coupled = coupling.astype(F32) if trail is None else exact_right(trail, coupling)
                for peer in range(leaves):
                    if peer >> depth != node ^ 1:
                        continue
                    entry = coupled
                    for lower in range(depth - 1, -1, -1):
                        entry = exact_right(entry, pt_ref[member, offsets[lower] + (peer >> lower)])
                    put(wide_ref, (member, rows, pl.ds((1 + peer) * rank, rank)), entry)
                trail = step.astype(F32) if trail is None else exact_right(trail, step)
            put(
                wide_ref,
                (member, rows, pl.ds((1 + leaf) * rank, rank)),
                jnp.zeros((rank, rank), F32),
            )
            put(wide_ref, (member, rows, pl.ds(0, rank)), exact_right(trail, qc_ref[member, own, 1]))
            below = exact_right(trail, qc_ref[member, own, 0])
            put(down_ref, (member, rows), below)
            feed = sign * mul(mm(vt_ref[other, leaf], u_ref[member, leaf]), below)
            put(feed_ref, (member, rows), feed)
            table = (
                up_ref[0, other, :, pl.ds(leaf * rank, rank)],
                up_ref[1, other, :, pl.ds(leaf * rank, rank)],
            )
            term = left_mul(table, feed)
            total = term if total is None else total + term
        chip_ref[2 * member] = total[:rank]
        chip_ref[2 * member + 1] = total[rank:].T


def far_table_kernel(plan, core_ref, qct_ref, top_ref, chip_ref, got_ref, *refs):
    lower_refs, (far_ref, sibling_ref) = refs[:-2], refs[-2:]
    rank = top_ref.shape[-1]
    for member in range(2):
        put(sibling_ref, (member,), got_ref[2 * member])
        loop = pieces(chip_ref[2 * member + 1] + got_ref[2 * member + 1])
        trail = None
        couplings = []
        levels = qct_ref.shape[1] + 1
        for level in range(levels):
            coupling = top_ref[member] if level == levels - 1 else qct_ref[member, level, 1]
            couplings.append(
                coupling.astype(F32) if trail is None else exact_left(coupling, trail)
            )
            if level < levels - 1:
                step = qct_ref[member, level, 0]
                trail = step.astype(F32) if trail is None else exact_left(step, trail)
        for index, (level, lower) in enumerate(plan):
            weight = couplings[level]
            if lower is not None:
                weight = exact_left(lower_refs[lower][member].astype(BF16), weight)
            rows = pl.ds(index * rank, rank)
            put(far_ref, (member, rows, slice(0, rank)), right_mul(weight, loop))
            put(far_ref, (member, rows, slice(rank, 2 * rank)), weight)


def stage_kernel(member, core_ref, table_ref, *refs):
    rank = table_ref.shape[-1]
    total = None
    for index, ref in enumerate(refs[:-1]):
        rows = pl.ds(index * rank, rank)
        term = right_mul(ref[...], (table_ref[0, member, rows], table_ref[1, member, rows]))
        total = term if total is None else total + term
    refs[-1][...] = total


def far_kernel(member, last, core_ref, table_ref, keep_ref, got_ref, *refs):
    count = len(refs) - (1 if last else 2)
    rank = table_ref.shape[-1] // 2
    total = None
    for index in range(count):
        rows = pl.ds(index * rank, rank)
        table = (table_ref[0, member, rows], table_ref[1, member, rows])
        term = right_mul(refs[index][...], table)
        total = term if total is None else total + term
    if not last:
        refs[count][...] = keep_ref[...] + got_ref[rank:] + total[:, :rank]
    refs[-1][...] = total[:, rank:]


def far_rows(core, mine_ref, theirs_ref):
    mine, theirs = mine_ref[...], theirs_ref[...]
    first = core == 0
    return jnp.concatenate(
        [jnp.where(first, mine, theirs), jnp.where(first, theirs, mine)], axis=0
    ).T


def expand(member, base, far):
    if member == 0:
        return exact_left(base, far)
    return mm(base, far.astype(BF16))


def local_kernel(member, leaves, first, *refs):
    refs = list(refs)
    core = refs.pop(0)[0]
    near_ref, u_ref, vt_ref, up_ref, wide_ref = (refs.pop(0) for _ in range(5))
    base_ref, other_ref, coef_ref, got_ref = (refs.pop(0) for _ in range(4))
    other = 1 - member
    rank = up_ref.shape[-1] // leaves
    rows = base_ref.shape[0] // leaves
    if first:
        coef = coef_ref[...]
        sibling = got_ref[:rank]
    else:
        down_ref, feed_ref, sibling_ref, mine_ref, theirs_ref = (refs.pop(0) for _ in range(5))
        far = far_rows(core, mine_ref, theirs_ref)
        coef = coef_ref[...] + left_mul((feed_ref[0, other], feed_ref[1, other]), far)
        sibling = got_ref[:rank] + left_mul((sibling_ref[0, other], sibling_ref[1, other]), far)
        leaf_far = left_mul((down_ref[0, other], down_ref[1, other]), far)
    out_ref, next_ref, send_ref, keep_ref = refs[:4]
    table = (wide_ref[0, member], wide_ref[1, member])
    inner = left_mul(table, jnp.concatenate([sibling, coef], axis=0))
    norm = None
    for leaf in range(leaves):
        part = slice(leaf * rows, (leaf + 1) * rows)
        small = slice(leaf * rank, (leaf + 1) * rank)
        value = base_ref[part]
        if not first:
            moved = expand(other, u_ref[other, leaf], leaf_far[small])
            value = value + moved if other == 1 else value - moved
            if other == 1:
                refs[4][part] = value
            else:
                term = jnp.sum(value * value, axis=0, keepdims=True)
                norm = term if norm is None else norm + term
        near = near_ref[member, leaf]
        if member == 0:
            result = exact_left(near, value)
        else:
            result = mm(near, value.astype(BF16))
        result = result + expand(member, u_ref[member, leaf], inner[small])
        if member == 0:
            result = other_ref[part] - result
        elif not first:
            result = other_ref[part] + result
        out_ref[part] = result
        if other == 0:
            next_ref[small] = exact_left(vt_ref[other, leaf], result)
        else:
            next_ref[small] = mm(vt_ref[other, leaf], result.astype(BF16))
    if norm is not None:
        refs[4][...] = norm
    lifted = left_mul((up_ref[0, other], up_ref[1, other]), next_ref[...])
    send_parts(core, lifted[:rank], lifted[rank:], send_ref, keep_ref)


def last_local_kernel(leaves, core_ref, near_ref, u_ref, vt_ref, up_ref, wide_ref, *refs):
    member, other = 1, 0
    base_ref, other_ref, coef_ref, got_ref = refs[:4]
    down_ref, feed_ref, sibling_ref, mine_ref, theirs_ref, out_ref, norm_ref = refs[4:]
    rank = up_ref.shape[-1] // leaves
    rows = base_ref.shape[0] // leaves
    far = far_rows(core_ref[0], mine_ref, theirs_ref)
    coef = coef_ref[...] + left_mul((feed_ref[0, other], feed_ref[1, other]), far)
    sibling = got_ref[:rank] + left_mul((sibling_ref[0, other], sibling_ref[1, other]), far)
    leaf_far = left_mul((down_ref[0, other], down_ref[1, other]), far)
    table = (wide_ref[0, member], wide_ref[1, member])
    inner = left_mul(table, jnp.concatenate([sibling, coef], axis=0))
    norm = None
    for leaf in range(leaves):
        part = slice(leaf * rows, (leaf + 1) * rows)
        small = slice(leaf * rank, (leaf + 1) * rank)
        value = base_ref[part] - expand(other, u_ref[other, leaf], leaf_far[small])
        term = jnp.sum(value * value, axis=0, keepdims=True)
        norm = term if norm is None else norm + term
        result = mm(near_ref[member, leaf], value.astype(BF16))
        result = result + expand(member, u_ref[member, leaf], inner[small])
        out_ref[part] = other_ref[part] + result
    norm_ref[...] = norm


def finish_kernel(leaves, core_ref, u_ref, down_ref, base_ref, mine_ref, theirs_ref, out_ref):
    rank = down_ref.shape[-1]
    rows = base_ref.shape[0] // leaves
    far = far_rows(core_ref[0], mine_ref, theirs_ref)
    leaf_far = left_mul((down_ref[0, 1], down_ref[1, 1]), far)
    for leaf in range(leaves):
        part = slice(leaf * rows, (leaf + 1) * rows)
        small = slice(leaf * rank, (leaf + 1) * rank)
        out_ref[part] = base_ref[part] + expand(1, u_ref[1, leaf], leaf_far[small])


def body(right_sides, near_blocks, leaf_bases, local_factors, upper_factors, top_couplings):
    bits_leaf = lax.axis_size("leaf").bit_length() - 1
    bits_rows = lax.axis_size("rows").bit_length() - 1
    levels_up = bits_leaf + bits_rows
    row_axis, leaf_size = lax.axis_size("rows"), lax.axis_size("leaf")
    leaves = near_blocks.shape[1]
    columns = right_sides.shape[1]
    rank = leaf_bases.shape[-1]
    half = columns // 2
    core = (lax.axis_index("leaf") % 2).astype(jnp.int32).reshape(1)
    top_position = lax.axis_index("rows") // 2 ** (bits_rows - 1) % 2

    def swap(value, mask):
        pairs = [(source, source ^ mask) for source in range(row_axis * leaf_size)]
        return lax.ppermute(value, ("rows", "leaf"), pairs)

    stages = []
    level = 1
    while level < levels_up:
        stages.append(tuple(range(level, min(level + 2, levels_up))))
        level += 2

    def masks_of(stage):
        low = 2 ** stage[0]
        return (low,) if len(stage) == 1 else (low, 2 * low, 3 * low)

    vt = jnp.swapaxes(leaf_bases[:, :, 1], -1, -2)
    u = leaf_bases[:, :, 0]
    pt = jnp.swapaxes(local_factors[:, :, 0], -1, -2)
    qc = local_factors[:, :, 1:]
    upper = upper_factors[:, 0]
    upper_p = upper[:, :, 0]
    qct = jnp.swapaxes(upper[:, :, 1:], -1, -2)
    top = lax.dynamic_index_in_dim(top_couplings, top_position, 1, keepdims=False)
    top = jnp.swapaxes(top, -1, -2)

    unit = rank * rank * columns
    up, coef, send, keep = call(
        functools.partial(start_kernel, leaves),
        [
            ((2, 2, 2 * rank, leaves * rank), BF16),
            ((leaves * rank, columns), F32),
            ((rank + half, rank), F32),
            ((half, rank), F32),
        ],
        [core, right_sides, vt, pt],
        150 * unit,
    )
    got = swap(send, 1)

    stage_tables, lower_refs, plan = [], [], []
    for stage in stages:
        low = 2 ** stage[0]
        base = stage[0] - 1
        if len(stage) == 1:
            plan.append((base, None))
            if stage[-1] == levels_up - 1:
                continue
        lower = upper_p[:, base].astype(F32)
        last = stage[-1] == levels_up - 1
        cross_got = swap(lower, 3 * low)
        if last:
            far_got = swap(lower, 2 * low)
        else:
            both = upper_p[:, base : base + 2].astype(F32)
            far_got = swap(
                jnp.swapaxes(both, 0, 1).reshape(4, rank, rank), 2 * low
            )
            near_got = swap(lower, low)
            stage_tables.append(
                call(
                    stage_table_kernel,
                    [((2, 2, 4 * rank, rank), BF16)],
                    [core, upper_p[:, base : base + 2], near_got, far_got, cross_got],
                    16 * unit,
                )[0]
            )
        plan.append((base, None))
        plan.append((base + 1, len(lower_refs)))
        plan.append((base + 1, len(lower_refs) + 1))
        lower_refs += [far_got, cross_got]

    wide, down, feed, chip_feed = call(
        functools.partial(local_table_kernel, leaves),
        [
            ((2, 2, leaves * rank, (leaves + 1) * rank), BF16),
            ((2, 2, leaves * rank, rank), BF16),
            ((2, 2, leaves * rank, rank), BF16),
            ((4, rank, rank), F32),
        ],
        [core, pt, qc, u, vt, up],
        300 * unit,
    )
    chip_got = swap(chip_feed, 1)
    far_table, sibling_table = call(
        functools.partial(far_table_kernel, plan),
        [((2, 2, len(plan) * rank, 2 * rank), BF16), ((2, 2, rank, rank), BF16)],
        [core, qct, top, chip_feed, chip_got] + lower_refs,
        100 * unit,
    )

    applies = 2 * STEPS + 1
    size = (right_sides.shape, F32)
    chip = keep + got[rank:]
    member = 1
    base = right_sides
    current = right_sides
    norms = []
    mine = theirs = None
    for index in range(applies):
        last = index == applies - 1
        shared = [core, near_blocks, u, vt, up, wide, base, current, coef, got]
        if index:
            shared += [down, feed, sibling_table, mine, theirs]
        arrived = []
        value = chip
        for number, stage in enumerate(stages):
            batch = [swap(value, mask) for mask in masks_of(stage)]
            arrived += batch
            if number < len(stages) - 1:
                value = call(
                    functools.partial(stage_kernel, member),
                    [((half, rank), F32)],
                    [core, stage_tables[number], value] + batch,
                    8 * unit,
                )[0]
        if last:
            base, norm = call(
                functools.partial(last_local_kernel, leaves),
                [size, ((1, columns), F32)],
                shared,
                200 * unit,
            )
            norms.append(norm)
        else:
            outs = [
                size,
                ((leaves * rank, columns), F32),
                ((rank + half, rank), F32),
                ((half, rank), F32),
            ]
            if index:
                outs.append(size if member == 0 else ((1, columns), F32))
            results = call(
                functools.partial(local_kernel, member, leaves, index == 0), outs, shared, 300 * unit
            )
            base, coef, send, keep = results[:4]
            got = swap(send, 1)
            if index and member == 0:
                current_solution = results[4]
            elif index:
                norms.append(results[4])
        outs = [((half, rank), F32)] * (1 if last else 2)
        results = call(
            functools.partial(far_kernel, member, last),
            outs,
            [core, far_table, keep, got] + arrived,
            20 * unit,
        )
        mine = results[-1]
        if not last:
            chip = results[0]
        theirs = swap(mine, 1)
        member = 1 - member
        if not last:
            current = right_sides if member == 0 else current_solution
    solution = call(
        functools.partial(finish_kernel, leaves),
        [size],
        [core, u, down, base, mine, theirs],
        30 * unit,
    )[0]
    norm_table = jnp.concatenate(norms)
    norm_table = norm_table + swap(norm_table, 1)
    for stage in stages:
        norm_table = sum([swap(norm_table, mask) for mask in masks_of(stage)], norm_table)
    return solution, norm_table


def solution(mesh):
    placed = (
        P(("rows", "leaf"), None),
        P(None, ("rows", "leaf"), None, None),
        P(None, ("rows", "leaf"), None, None, None),
        P(None, ("rows", "leaf"), None, None, None),
        P(None, ("rows", "leaf"), None, None, None, None),
        P(),
    )
    return jax.shard_map(
        body,
        mesh=mesh,
        in_specs=placed,
        out_specs=(P(("rows", "leaf"), None), P()),
        check_vma=False,
    )
```

```python
import functools

import jax
import jax.numpy as jnp
from jax import lax
from jax.experimental import pallas as pl
from jax.experimental.pallas import tpu as pltpu
from jax.sharding import PartitionSpec as P


STEPS = 3
BF16 = jnp.bfloat16
F32 = jnp.float32
VMEM_LIMIT = 16 * 2**20
START_LIMIT = 50 * 2**20


def mm(left, right):
    return jnp.dot(left, right, preferred_element_type=F32)


def pieces(value):
    high = value.astype(BF16)
    return high, (value - high.astype(F32)).astype(BF16)


def left_mul(table, value):
    high, low = pieces(value)
    width = value.shape[1]
    both = mm(table[0], jnp.concatenate([high, low], axis=1))
    return both[:, :width] + both[:, width:] + mm(table[1], high)


def right_mul(value, table):
    high, low = pieces(value)
    rows = value.shape[0]
    both = mm(jnp.concatenate([high, low], axis=0), table[0])
    return both[:rows] + both[rows:] + mm(high, table[1])


def mul(left, right):
    return left_mul(pieces(left), right)


def exact_left(table, value):
    high, low = pieces(value)
    width = value.shape[1]
    both = mm(table, jnp.concatenate([high, low], axis=1))
    return both[:, :width] + both[:, width:]


def exact_right(value, table):
    high, low = pieces(value)
    rows = value.shape[0]
    both = mm(jnp.concatenate([high, low], axis=0), table)
    return both[:rows] + both[rows:]


def put(ref, index, value):
    high, low = pieces(value)
    ref[(0,) + index] = high
    ref[(1,) + index] = low


def call(kernel, outs, args, flops, hbm=False, scratch=()):
    specs = [pl.BlockSpec(memory_space=pltpu.HBM if hbm else pltpu.VMEM)] * len(args)
    return pl.pallas_call(
        kernel,
        out_shape=[jax.ShapeDtypeStruct(shape, dtype) for shape, dtype in outs],
        in_specs=specs,
        out_specs=[pl.BlockSpec(memory_space=pltpu.VMEM)] * len(outs),
        scratch_shapes=list(scratch),
        compiler_params=pltpu.CompilerParams(vmem_limit_bytes=START_LIMIT if hbm else VMEM_LIMIT),
        cost_estimate=pl.CostEstimate(flops=flops, bytes_accessed=0, transcendentals=0),
    )(*args)


def level_offsets(leaf_count):
    offsets, count, offset = [], leaf_count, 0
    while count >= 1:
        offsets.append(offset)
        offset += count
        count //= 2
    return offsets


def send_parts(device, lifted, send_ref, keep_ref):
    columns = lifted.shape[1]
    half = columns // 2
    turned = lifted.T
    first = lax.axis_index("leaf") % 2 == 0
    keep_ref[...] = jnp.where(first, turned[:half], turned[half:])
    send_ref[: device.shape[0]] = device
    send_ref[device.shape[0] :] = jnp.where(first, turned[half:], turned[:half])


def start_kernel(leaves, *refs):
    right_hbm, near_hbm, bases_hbm, local_hbm, upper_hbm, top_hbm = refs[:6]
    right_ref, near_ref, bases_ref, local_ref, upper_ref, top_ref = refs[6:12]
    vt_ref, up_ref, coef_ref, send_ref, keep_ref, semaphores = refs[12:]
    position = lax.axis_index("rows") // (lax.axis_size("rows") // 2)
    copies = [
        pltpu.make_async_copy(source, target, semaphores.at[index])
        for index, (source, target) in enumerate(
            [
                (local_hbm, local_ref),
                (bases_hbm, bases_ref),
                (right_hbm, right_ref),
                (upper_hbm.at[:, 0], upper_ref),
                (top_hbm.at[:, position], top_ref),
                (near_hbm, near_ref),
            ]
        )
    ]
    for copy in copies:
        copy.start()
    copies[0].wait()
    rank = local_ref.shape[-1]
    up_table(1, leaves, local_ref, up_ref)
    copies[1].wait()
    copies[2].wait()
    rows = right_ref.shape[0] // leaves
    for leaf in range(leaves):
        turned = bases_ref[1, leaf, 1].T
        vt_ref[leaf] = turned
        value = right_ref[leaf * rows : (leaf + 1) * rows].astype(BF16)
        coef_ref[leaf * rank : (leaf + 1) * rank] = mm(turned, value)
    lifted = left_mul((up_ref[0], up_ref[1]), coef_ref[...])
    send_parts(lifted[:rank], lifted[rank:], send_ref, keep_ref)
    for copy in copies[3:]:
        copy.wait()


def up_table(member, leaves, local_ref, up_ref):
    rank = local_ref.shape[-1]
    offsets = level_offsets(leaves)
    turned = {}

    def transfer(node):
        if node not in turned:
            turned[node] = local_ref[member, node, 0].T
        return turned[node]

    for leaf in range(leaves):
        trail = transfer(leaf).astype(F32)
        for depth in range(1, len(offsets)):
            if depth == len(offsets) - 1:
                put(up_ref, (slice(0, rank), pl.ds(leaf * rank, rank)), trail)
            trail = exact_left(transfer(offsets[depth] + (leaf >> depth)), trail)
        put(up_ref, (slice(rank, 2 * rank), pl.ds(leaf * rank, rank)), trail)


def pack_kernel(base, last, upper_ref, *refs):
    near_ref, far_ref, cross_ref = refs[-3:]
    half = near_ref.shape[0] if last else near_ref.shape[0] - 2 * upper_ref.shape[-1]
    rank = upper_ref.shape[-1]
    value = refs[0][...]
    if len(refs) == 5:
        value = value + refs[1][rank:]
    for ref in (near_ref, far_ref, cross_ref):
        ref[:half] = value
    for member in range(2):
        lower = upper_ref[member, base, 0].astype(F32)
        rows = pl.ds(half + member * rank, rank)
        far_ref[rows] = lower
        cross_ref[rows] = lower
        if not last:
            near_ref[rows] = lower
            far_ref[pl.ds(half + (2 + member) * rank, rank)] = upper_ref[
                member, base + 1, 0
            ].astype(F32)


def stage_table_kernel(base, upper_ref, near_ref, far_ref, cross_ref, out_ref):
    rank = upper_ref.shape[-1]
    half = near_ref.shape[0] - 2 * rank
    for member in range(2):
        rows = pl.ds(half + member * rank, rank)
        here = upper_ref[member, base + 1, 0]
        there = far_ref[pl.ds(half + (2 + member) * rank, rank)].astype(BF16)
        lowers = [upper_ref[member, base, 0]]
        lowers += [ref[rows].astype(BF16) for ref in (near_ref, far_ref, cross_ref)]
        for index, (lower, upper) in enumerate(zip(lowers, (here, here, there, there))):
            put(out_ref, (member, pl.ds(index * rank, rank)), mm(lower, upper))


def local_table_kernel(leaves, local_ref, bases_ref, vt1_ref, up1_ref, *refs):
    vt0_ref, up0_ref, wide_ref, down_ref, feed_ref, chip_ref = refs
    vt_refs, up_refs = (vt0_ref, vt1_ref), (up0_ref, up1_ref)
    rank = local_ref.shape[-1]
    offsets = level_offsets(leaves)
    own = offsets[-1]
    up_table(0, leaves, local_ref, up0_ref)
    for leaf in range(leaves):
        vt0_ref[leaf] = bases_ref[0, leaf, 1].T
    for member in (1, 0):
        other = 1 - member
        sign = 1.0 if member == 1 else -1.0
        total = None
        turned = {}

        def transfer(node):
            if node not in turned:
                turned[node] = local_ref[member, node, 0].T
            return turned[node]

        for leaf in range(leaves):
            rows = pl.ds(leaf * rank, rank)
            trail = None
            for depth in range(len(offsets) - 1):
                node = leaf >> depth
                step = local_ref[member, offsets[depth] + node, 1]
                coupling = local_ref[member, offsets[depth] + node, 2]
                coupled = coupling.astype(F32) if trail is None else exact_right(trail, coupling)
                for peer in range(leaves):
                    if peer >> depth != node ^ 1:
                        continue
                    entry = coupled
                    for lower in range(depth - 1, -1, -1):
                        entry = exact_right(entry, transfer(offsets[lower] + (peer >> lower)))
                    put(wide_ref, (member, rows, pl.ds((1 + peer) * rank, rank)), entry)
                trail = step.astype(F32) if trail is None else exact_right(trail, step)
            put(
                wide_ref,
                (member, rows, pl.ds((1 + leaf) * rank, rank)),
                jnp.zeros((rank, rank), F32),
            )
            put(
                wide_ref,
                (member, rows, pl.ds(0, rank)),
                exact_right(trail, local_ref[member, own, 2]),
            )
            below = exact_right(trail, local_ref[member, own, 1])
            put(down_ref, (member, rows), below)
            feed = sign * mul(mm(vt_refs[other][leaf], bases_ref[member, leaf, 0]), below)
            put(feed_ref, (member, rows), feed)
            table = tuple(
                up_refs[other][piece, :, pl.ds(leaf * rank, rank)] for piece in range(2)
            )
            term = left_mul(table, feed)
            total = term if total is None else total + term
        chip_ref[2 * member] = total[:rank]
        chip_ref[2 * member + 1] = total[rank:].T


def far_table_kernel(plan, half, upper_ref, top_ref, chip_ref, got_ref, *refs):
    lower_refs, (far_ref, sibling_ref) = refs[:-2], refs[-2:]
    rank = top_ref.shape[-1]
    for member in range(2):
        put(sibling_ref, (member,), got_ref[2 * member])
        loop = pieces(chip_ref[2 * member + 1] + got_ref[2 * member + 1])
        trail = None
        couplings = []
        levels = upper_ref.shape[1] + 1
        for level in range(levels):
            coupling = top_ref[member] if level == levels - 1 else upper_ref[member, level, 2]
            coupling = coupling.T
            couplings.append(
                coupling.astype(F32) if trail is None else exact_left(coupling, trail)
            )
            if level < levels - 1:
                step = upper_ref[member, level, 1].T
                trail = step.astype(F32) if trail is None else exact_left(step, trail)
        for index, (level, lower) in enumerate(plan):
            weight = couplings[level]
            if lower is not None:
                transfer = lower_refs[lower][pl.ds(half + member * rank, rank)]
                weight = exact_left(transfer.astype(BF16), weight)
            rows = pl.ds(index * rank, rank)
            put(far_ref, (member, rows, slice(0, rank)), right_mul(weight, loop))
            put(far_ref, (member, rows, slice(rank, 2 * rank)), weight)


def stage_kernel(member, half, table_ref, *refs):
    rank = table_ref.shape[-1]
    total = None
    for index in range(4):
        rows = pl.ds(index * rank, rank)
        table = (table_ref[0, member, rows], table_ref[1, member, rows])
        term = right_mul(refs[index][:half], table)
        total = term if total is None else total + term
    refs[-1][:half] = total
    if len(refs) > 5:
        refs[-1][half:] = refs[4][...] + refs[5][...]


def far_kernel(member, last, table_ref, keep_ref, got_ref, *refs):
    rank = table_ref.shape[-1] // 2
    half = refs[-1].shape[0]
    count = len(refs) - 2
    total = None
    for index in range(count):
        rows = pl.ds(index * rank, rank)
        table = (table_ref[0, member, rows], table_ref[1, member, rows])
        term = right_mul(refs[index][:half], table)
        total = term if total is None else total + term
    if not last:
        refs[count][...] = keep_ref[...] + got_ref[rank:] + total[:, :rank]
    else:
        sums = None
        for ref in refs[:count]:
            if ref.shape[0] == half + 8:
                sums = ref[half:] if sums is None else sums + ref[half:]
        refs[count][...] = sums
    refs[-1][...] = total[:, rank:]


def far_rows(mine_ref, theirs_ref):
    mine, theirs = mine_ref[...], theirs_ref[...]
    first = lax.axis_index("leaf") % 2 == 0
    return jnp.concatenate(
        [jnp.where(first, mine, theirs), jnp.where(first, theirs, mine)], axis=0
    ).T


def expand(member, base, far):
    if member == 0:
        return exact_left(base, far)
    return mm(base, far.astype(BF16))


def local_kernel(member, leaves, first, *refs):
    refs = list(refs)
    near_ref, bases_ref, vt_ref, up_ref, wide_ref = (refs.pop(0) for _ in range(5))
    base_ref, other_ref, coef_ref, got_ref = (refs.pop(0) for _ in range(4))
    other = 1 - member
    rank = up_ref.shape[-1] // leaves
    rows = base_ref.shape[0] // leaves
    if first:
        coef = coef_ref[...]
        sibling = got_ref[:rank]
    else:
        down_ref, feed_ref, sibling_ref, mine_ref, theirs_ref = (refs.pop(0) for _ in range(5))
        far = far_rows(mine_ref, theirs_ref)
        coef = coef_ref[...] + left_mul((feed_ref[0, other], feed_ref[1, other]), far)
        sibling = got_ref[:rank] + left_mul((sibling_ref[0, other], sibling_ref[1, other]), far)
        leaf_far = left_mul((down_ref[0, other], down_ref[1, other]), far)
    out_ref, next_ref, send_ref, keep_ref = refs[:4]
    table = (wide_ref[0, member], wide_ref[1, member])
    inner = left_mul(table, jnp.concatenate([sibling, coef], axis=0))
    norm = None
    for leaf in range(leaves):
        part = slice(leaf * rows, (leaf + 1) * rows)
        small = slice(leaf * rank, (leaf + 1) * rank)
        value = base_ref[part]
        if not first:
            moved = expand(other, bases_ref[other, leaf, 0], leaf_far[small])
            value = value + moved if other == 1 else value - moved
            if other == 1:
                refs[4][part] = value
            else:
                term = jnp.sum(value * value, axis=0, keepdims=True)
                norm = term if norm is None else norm + term
        near = near_ref[member, leaf]
        if member == 0:
            result = exact_left(near, value)
        else:
            result = mm(near, value.astype(BF16))
        result = result + expand(member, bases_ref[member, leaf, 0], inner[small])
        if member == 0:
            result = other_ref[part] - result
        elif not first:
            result = other_ref[part] + result
        out_ref[part] = result
        if other == 0:
            next_ref[small] = exact_left(vt_ref[leaf], result)
        else:
            next_ref[small] = mm(vt_ref[leaf], result.astype(BF16))
    if norm is not None:
        refs[4][...] = norm
    lifted = left_mul((up_ref[0], up_ref[1]), next_ref[...])
    send_parts(lifted[:rank], lifted[rank:], send_ref, keep_ref)


def last_local_kernel(leaves, near_ref, bases_ref, vt_ref, up_ref, wide_ref, *refs):
    member, other = 1, 0
    base_ref, other_ref, coef_ref, got_ref = refs[:4]
    down_ref, feed_ref, sibling_ref, mine_ref, theirs_ref = refs[4:9]
    *old_refs, out_ref, norm_ref = refs[9:]
    rank = up_ref.shape[-1] // leaves
    rows = base_ref.shape[0] // leaves
    far = far_rows(mine_ref, theirs_ref)
    coef = coef_ref[...] + left_mul((feed_ref[0, other], feed_ref[1, other]), far)
    sibling = got_ref[:rank] + left_mul((sibling_ref[0, other], sibling_ref[1, other]), far)
    leaf_far = left_mul((down_ref[0, other], down_ref[1, other]), far)
    table = (wide_ref[0, member], wide_ref[1, member])
    inner = left_mul(table, jnp.concatenate([sibling, coef], axis=0))
    norm = None
    for leaf in range(leaves):
        part = slice(leaf * rows, (leaf + 1) * rows)
        small = slice(leaf * rank, (leaf + 1) * rank)
        value = base_ref[part] - expand(other, bases_ref[other, leaf, 0], leaf_far[small])
        term = jnp.sum(value * value, axis=0, keepdims=True)
        norm = term if norm is None else norm + term
        result = mm(near_ref[member, leaf], value.astype(BF16))
        result = result + expand(member, bases_ref[member, leaf, 0], inner[small])
        out_ref[part] = other_ref[part] + result
    norm_ref[...] = jnp.zeros_like(norm_ref)
    for index, ref in enumerate(old_refs):
        norm_ref[index : index + 1] = ref[...]
    norm_ref[len(old_refs) : len(old_refs) + 1] = norm


def finish_kernel(leaves, bases_ref, down_ref, base_ref, mine_ref, theirs_ref, out_ref):
    rank = down_ref.shape[-1]
    rows = base_ref.shape[0] // leaves
    far = far_rows(mine_ref, theirs_ref)
    leaf_far = left_mul((down_ref[0, 1], down_ref[1, 1]), far)
    for leaf in range(leaves):
        part = slice(leaf * rows, (leaf + 1) * rows)
        small = slice(leaf * rank, (leaf + 1) * rank)
        out_ref[part] = base_ref[part] + expand(1, bases_ref[1, leaf, 0], leaf_far[small])


def body(right_sides, near_blocks, leaf_bases, local_factors, upper_factors, top_couplings):
    bits_leaf = lax.axis_size("leaf").bit_length() - 1
    bits_rows = lax.axis_size("rows").bit_length() - 1
    devices = lax.axis_size("rows") * lax.axis_size("leaf")
    leaves = near_blocks.shape[1]
    columns = right_sides.shape[1]
    rank = leaf_bases.shape[-1]
    half = columns // 2
    stages = stages_of(bits_leaf + bits_rows)

    def swap(value, mask):
        pairs = [(source, source ^ mask) for source in range(devices)]
        return lax.ppermute(value, ("rows", "leaf"), pairs)

    unit = 2 * rank * rank * columns
    message = ((half, rank), F32)
    lifted = ((rank + half, rank), F32)
    coefs = ((leaves * rank, columns), F32)
    size = (right_sides.shape, F32)
    uppers = (2,) + upper_factors.shape[2:]
    loaded = call(
        functools.partial(start_kernel, leaves),
        [
            size,
            (near_blocks.shape, BF16),
            (leaf_bases.shape, BF16),
            (local_factors.shape, BF16),
            (uppers, BF16),
            ((2, rank, rank), BF16),
            ((leaves, rank, leaf_bases.shape[3]), BF16),
            ((2, 2 * rank, leaves * rank), BF16),
            coefs,
            lifted,
            message,
        ],
        [right_sides, near_blocks, leaf_bases, local_factors, upper_factors, top_couplings],
        150 * unit,
        hbm=True,
        scratch=[pltpu.SemaphoreType.DMA((6,))],
    )
    right, near, bases, local, upper, top, vt_inverse, up_inverse, coef, send, keep = loaded
    got = swap(send, 1)

    vt = [None, vt_inverse]
    up = [None, up_inverse]
    stage_tables, lower_refs, plan = [], [], []
    member = 1
    base = current = right
    chip = None
    norms = []
    mine = theirs = None
    applies = 2 * STEPS + 1
    for index in range(applies):
        last = index == applies - 1
        arrived = []
        value = chip
        norm = None
        for number, stage in enumerate(stages):
            low = 2 ** stage[0]
            lower_level = stage[0] - 1
            top_stage = number == len(stages) - 1
            masks = (low,) if len(stage) == 1 else (low, 2 * low, 3 * low)
            sent = [value] * len(masks)
            if index == 0 and len(stage) > 1:
                tall = (half + 2 * rank, rank)
                sent = call(
                    functools.partial(pack_kernel, lower_level, top_stage),
                    [
                        message if top_stage else (tall, F32),
                        (tall if top_stage else (half + 4 * rank, rank), F32),
                        (tall, F32),
                    ],
                    [upper] + ([value] if number else [keep, got]),
                    unit,
                )
                value = sent[0]
            elif index == 0 and value is None:
                value = keep + got[rank:]
                sent = [value] * len(masks)
            batch = [swap(data, mask) for data, mask in zip(sent, masks)]
            arrived += batch
            if index == 0:
                plan.append((lower_level, None))
                if len(stage) > 1:
                    plan.append((lower_level + 1, len(lower_refs)))
                    plan.append((lower_level + 1, len(lower_refs) + 1))
                    lower_refs += batch[1:]
                if not top_stage:
                    stage_tables += call(
                        functools.partial(stage_table_kernel, lower_level),
                        [((2, 2, 4 * rank, rank), BF16)],
                        [upper] + batch,
                        16 * unit,
                    )
            if number == 0:
                if index == 0:
                    tables = call(
                        functools.partial(local_table_kernel, leaves),
                        [
                            ((leaves, rank, leaf_bases.shape[3]), BF16),
                            ((2, 2 * rank, leaves * rank), BF16),
                            ((2, 2, leaves * rank, (leaves + 1) * rank), BF16),
                            ((2, 2, leaves * rank, rank), BF16),
                            ((2, 2, leaves * rank, rank), BF16),
                            ((4, rank, rank), F32),
                        ],
                        [local, bases, vt_inverse, up_inverse],
                        300 * unit,
                    )
                    vt[0], up[0], wide, down, feed, chip_feed = tables
                    chip_got = swap(chip_feed, 1)
                other = 1 - member
                shared = [near, bases, vt[other], up[other], wide, base, current, coef, got]
                if index:
                    shared += [down, feed, sibling_table, mine, theirs]
                if last:
                    base, norm = call(
                        functools.partial(last_local_kernel, leaves),
                        [size, ((8, columns), F32)],
                        shared + norms,
                        200 * unit,
                    )
                    norm_got = swap(norm, 1)
                else:
                    outs = [size, coefs, lifted, message]
                    if index:
                        outs.append(size if member == 0 else ((1, columns), F32))
                    results = call(
                        functools.partial(local_kernel, member, leaves, index == 0),
                        outs,
                        shared,
                        300 * unit,
                    )
                    base, coef, send, next_keep = results[:4]
                    next_got = swap(send, 1)
                    if index and member == 0:
                        iterate = results[4]
                    elif index:
                        norms.append(results[4])
            if not top_stage:
                extra = [norm, norm_got] if last and number == len(stages) - 2 else []
                args = [value] + batch + extra
                shape = (half + (8 if extra else 0), rank)
                value = call(
                    functools.partial(stage_kernel, member, half),
                    [(shape, F32)],
                    [stage_tables[number]] + args,
                    8 * unit,
                )[0]
        if index == 0:
            far_table, sibling_table = call(
                functools.partial(far_table_kernel, plan, half),
                [((2, 2, len(plan) * rank, 2 * rank), BF16), ((2, 2, rank, rank), BF16)],
                [upper, top, chip_feed, chip_got] + lower_refs,
                100 * unit,
            )
        results = call(
            functools.partial(far_kernel, member, last),
            [((8, columns), F32) if last else message, message],
            [far_table] + ([keep, got] if last else [next_keep, next_got]) + arrived,
            20 * unit,
        )
        chip, mine = results
        theirs = swap(mine, 1)
        if last:
            sums = chip + value[half:]
        else:
            keep, got = next_keep, next_got
        member = 1 - member
        if not last:
            current = right if member == 0 else iterate
    solution = call(
        functools.partial(finish_kernel, leaves),
        [size],
        [bases, down, base, mine, theirs],
        30 * unit,
    )[0]
    for stage in stages[:-1]:
        low = 2 ** stage[0]
        masks = (low,) if len(stage) == 1 else (low, 2 * low, 3 * low)
        sums = sum([swap(sums, mask) for mask in masks], sums)
    return solution, sums[:STEPS]


def stages_of(levels_up):
    return [tuple(range(level, min(level + 2, levels_up))) for level in range(1, levels_up, 2)]


def solution(mesh):
    placed = (
        P(("rows", "leaf"), None),
        P(None, ("rows", "leaf"), None, None),
        P(None, ("rows", "leaf"), None, None, None),
        P(None, ("rows", "leaf"), None, None, None),
        P(None, ("rows", "leaf"), None, None, None, None),
        P(),
    )

    return jax.shard_map(
        body,
        mesh=mesh,
        in_specs=placed,
        out_specs=(P(("rows", "leaf"), None), P()),
        check_vma=False,
    )
```

```python
import functools

import jax
import jax.numpy as jnp
from jax import lax
from jax.experimental import pallas as pl
from jax.experimental.pallas import tpu as pltpu
from jax.sharding import PartitionSpec as P


STEPS = 3
BF16 = jnp.bfloat16
F32 = jnp.float32
VMEM_LIMIT = 16 * 2**20
START_LIMIT = 48 * 2**20


def mm(left, right):
    return jnp.dot(left, right, preferred_element_type=F32)


def pieces(value):
    high = value.astype(BF16)
    return high, (value - high.astype(F32)).astype(BF16)


def left_mul(table, value):
    high, low = pieces(value)
    width = value.shape[1]
    both = mm(table[0], jnp.concatenate([high, low], axis=1))
    return both[:, :width] + both[:, width:] + mm(table[1], high)


def right_mul(value, table):
    high, low = pieces(value)
    rows = value.shape[0]
    both = mm(jnp.concatenate([high, low], axis=0), table[0])
    return both[:rows] + both[rows:] + mm(high, table[1])


def mul(left, right):
    return left_mul(pieces(left), right)


def exact_left(table, value):
    high, low = pieces(value)
    width = value.shape[1]
    both = mm(table, jnp.concatenate([high, low], axis=1))
    return both[:, :width] + both[:, width:]


def exact_right(value, table):
    high, low = pieces(value)
    rows = value.shape[0]
    both = mm(jnp.concatenate([high, low], axis=0), table)
    return both[:rows] + both[rows:]


def put(ref, index, value):
    high, low = pieces(value)
    ref[(0,) + index] = high
    ref[(1,) + index] = low


def call(kernel, outs, args, flops, hbm=False, scratch=()):
    specs = [pl.BlockSpec(memory_space=pltpu.HBM if hbm else pltpu.VMEM)] * len(args)
    return pl.pallas_call(
        kernel,
        out_shape=[jax.ShapeDtypeStruct(shape, dtype) for shape, dtype in outs],
        in_specs=specs,
        out_specs=[pl.BlockSpec(memory_space=pltpu.VMEM)] * len(outs),
        scratch_shapes=list(scratch),
        compiler_params=pltpu.CompilerParams(vmem_limit_bytes=START_LIMIT if hbm else VMEM_LIMIT),
        cost_estimate=pl.CostEstimate(flops=flops, bytes_accessed=0, transcendentals=0),
    )(*args)


def level_offsets(leaf_count):
    offsets, count, offset = [], leaf_count, 0
    while count >= 1:
        offsets.append(offset)
        offset += count
        count //= 2
    return offsets


def send_parts(device, lifted, send_ref, keep_ref):
    columns = lifted.shape[1]
    half = columns // 2
    turned = lifted.T
    first = lax.axis_index("leaf") % 2 == 0
    keep_ref[...] = jnp.where(first, turned[:half], turned[half:])
    send_ref[: device.shape[0]] = device
    send_ref[device.shape[0] :] = jnp.where(first, turned[half:], turned[:half])


def start_kernel(leaves, *refs):
    right_hbm, bases_hbm, local_hbm = refs[:3]
    upper_rows_ref, lower_rows_ref, u0_ref, u1_ref, v0_ref, local0_ref, local1_ref = refs[3:10]
    vt_ref, up_ref, coef_ref, send_ref, keep_ref, v1_ref, semaphores = refs[10:]
    rows = right_hbm.shape[0] // leaves
    middle = right_hbm.shape[0] // 2
    copies = [
        pltpu.make_async_copy(source, target, semaphores.at[index])
        for index, (source, target) in enumerate(
            [
                (local_hbm.at[1], local1_ref),
                (bases_hbm.at[1, :, 1], v1_ref),
                (right_hbm.at[:middle], upper_rows_ref),
                (right_hbm.at[middle:], lower_rows_ref),
                (local_hbm.at[0], local0_ref),
                (bases_hbm.at[0, :, 1], v0_ref),
                (bases_hbm.at[1, :, 0], u1_ref),
                (bases_hbm.at[0, :, 0], u0_ref),
            ]
        )
    ]
    for copy in copies:
        copy.start()
    copies[0].wait()
    rank = local1_ref.shape[-1]
    up_table(leaves, local1_ref, up_ref)
    copies[1].wait()
    for leaf in range(leaves):
        vt_ref[leaf] = v1_ref[leaf].T
    copies[2].wait()
    copies[3].wait()
    for leaf in range(leaves):
        value = rows_of((upper_rows_ref, lower_rows_ref), leaf, rows).astype(BF16)
        coef_ref[leaf * rank : (leaf + 1) * rank] = mm(vt_ref[leaf], value)
    lifted = left_mul((up_ref[0], up_ref[1]), coef_ref[...])
    send_parts(lifted[:rank], lifted[rank:], send_ref, keep_ref)
    for copy in copies[4:]:
        copy.wait()


def rows_of(refs, leaf, rows):
    held = refs[0].shape[0] // rows
    place = (leaf % held) * rows
    return refs[leaf // held][place : place + rows]


def up_table(leaves, local_ref, up_ref):
    rank = local_ref.shape[-1]
    offsets = level_offsets(leaves)
    turned = {}

    def transfer(node):
        if node not in turned:
            turned[node] = local_ref[node, 0].T
        return turned[node]

    for leaf in range(leaves):
        trail = transfer(leaf).astype(F32)
        for depth in range(1, len(offsets)):
            if depth == len(offsets) - 1:
                put(up_ref, (slice(0, rank), pl.ds(leaf * rank, rank)), trail)
            trail = exact_left(transfer(offsets[depth] + (leaf >> depth)), trail)
        put(up_ref, (slice(rank, 2 * rank), pl.ds(leaf * rank, rank)), trail)


def pack_kernel(base, last, upper_ref, *refs):
    near_ref, far_ref, cross_ref = refs[-3:]
    half = cross_ref.shape[0]
    rank = upper_ref.shape[-1]
    value = refs[0][...]
    if len(refs) == 5:
        value = value + refs[1][rank:]
    risen = exact_right(value, upper_ref[1, base, 0])
    near_ref[:half] = value
    far_ref[:half] = risen
    cross_ref[...] = risen
    if not last:
        for member in range(2):
            rows = pl.ds(half + member * rank, rank)
            near_ref[rows] = upper_ref[member, base, 0].astype(F32)
            far_ref[rows] = upper_ref[member, base + 1, 0].astype(F32)


def stage_table_kernel(base, half, upper_ref, near_ref, far_ref, out_ref):
    rank = upper_ref.shape[-1]
    for member in range(2):
        rows = pl.ds(half + member * rank, rank)
        here = upper_ref[member, base + 1, 0]
        put(out_ref, (member, pl.ds(0, rank)), mm(upper_ref[member, base, 0], here))
        put(out_ref, (member, pl.ds(rank, rank)), mm(near_ref[rows].astype(BF16), here))
        put(out_ref, (member, pl.ds(2 * rank, rank)), far_ref[rows])


def local_table_kernel(leaves, *refs):
    local_refs, u_refs = refs[0:2], refs[2:4]
    v0_ref, vt1_ref, up1_ref, vt0_ref, up0_ref, wide_ref, down_ref, feed_ref, chip_ref = refs[4:]
    vt_refs, up_refs = (vt0_ref, vt1_ref), (up0_ref, up1_ref)
    rank = up1_ref.shape[-1] // leaves
    offsets = level_offsets(leaves)
    own = offsets[-1]
    up_table(leaves, local_refs[0], up0_ref)
    for leaf in range(leaves):
        vt0_ref[leaf] = v0_ref[leaf].T
    for member in (1, 0):
        other = 1 - member
        local_ref = local_refs[member]
        sign = 1.0 if member == 1 else -1.0
        total = None
        turned = {}

        def transfer(node):
            if node not in turned:
                turned[node] = local_ref[node, 0].T
            return turned[node]

        for leaf in range(leaves):
            rows = pl.ds(leaf * rank, rank)
            trail = None
            for depth in range(len(offsets) - 1):
                node = leaf >> depth
                step = local_ref[offsets[depth] + node, 1]
                coupling = local_ref[offsets[depth] + node, 2]
                coupled = coupling.astype(F32) if trail is None else exact_right(trail, coupling)
                for peer in range(leaves):
                    if peer >> depth != node ^ 1:
                        continue
                    entry = coupled
                    for lower in range(depth - 1, -1, -1):
                        entry = exact_right(entry, transfer(offsets[lower] + (peer >> lower)))
                    put(wide_ref, (member, rows, pl.ds((1 + peer) * rank, rank)), entry)
                trail = step.astype(F32) if trail is None else exact_right(trail, step)
            put(
                wide_ref,
                (member, rows, pl.ds((1 + leaf) * rank, rank)),
                jnp.zeros((rank, rank), F32),
            )
            put(
                wide_ref,
                (member, rows, pl.ds(0, rank)),
                exact_right(trail, local_ref[own, 2]),
            )
            below = exact_right(trail, local_ref[own, 1])
            put(down_ref, (member, rows), below)
            feed = sign * mul(mm(vt_refs[other][leaf], u_refs[member][leaf]), below)
            put(feed_ref, (member, rows), feed)
            table = tuple(
                up_refs[other][piece, :, pl.ds(leaf * rank, rank)] for piece in range(2)
            )
            term = left_mul(table, feed)
            total = term if total is None else total + term
        chip_ref[2 * member] = total[:rank]
        chip_ref[2 * member + 1] = total[rank:].T


def far_table_kernel(upper_ref, top_ref, chip_ref, got_ref, far_ref, sibling_ref):
    position = lax.axis_index("rows") // (lax.axis_size("rows") // 2)
    rank = top_ref.shape[-1]
    for member in range(2):
        put(sibling_ref, (member,), got_ref[2 * member])
        loop = pieces(chip_ref[2 * member + 1] + got_ref[2 * member + 1])
        trail = None
        levels = upper_ref.shape[1] + 1
        for level in range(levels):
            if level == levels - 1:
                coupling = jnp.where(position == 0, top_ref[member, 0], top_ref[member, 1])
            else:
                coupling = upper_ref[member, level, 2]
            coupling = coupling.T
            weight = coupling.astype(F32) if trail is None else exact_left(coupling, trail)
            if level < levels - 1:
                step = upper_ref[member, level, 1].T
                trail = step.astype(F32) if trail is None else exact_left(step, trail)
            rows = pl.ds(level * rank, rank)
            put(far_ref, (member, rows, slice(0, rank)), right_mul(weight, loop))
            put(far_ref, (member, rows, slice(rank, 2 * rank)), weight)


def rows_table(table_ref, member, index, rank):
    rows = pl.ds(index * rank, rank)
    return (table_ref[0, member, rows], table_ref[1, member, rows])


def stage_kernel(member, half, lift, upper_ref, table_ref, own_ref, *refs):
    near_ref, far_ref, cross_ref = refs[:3]
    rank = table_ref.shape[-1]
    total = right_mul(own_ref[:half], rows_table(table_ref, member, 0, rank))
    total = total + right_mul(near_ref[:half], rows_table(table_ref, member, 1, rank))
    both = far_ref[:half] + cross_ref[:half]
    total = total + exact_right(both, table_ref[0, member, pl.ds(2 * rank, rank)])
    outs = refs[3:]
    if lift is None:
        outs = outs[-1:]
    elif len(outs) > 2:
        outs = outs[-2:]
    outs[0][:half] = total
    if lift is not None:
        outs[1][:half] = exact_right(total, upper_ref[member, lift, 0])
    if outs[0].shape[0] > half:
        for ref in outs:
            ref[half:] = refs[3][...] + refs[4][...]


def far_kernel(member, last, plan, half, upper_ref, table_ref, keep_ref, got_ref, *refs):
    rank = table_ref.shape[-1] // 2
    total = None
    count = sum(plan)
    place = level = 0
    for size in plan:
        parts = [refs[place][:half]]
        if size == 3:
            parts.append(refs[place + 1][:half] + refs[place + 2][:half])
        for part in parts:
            term = right_mul(part, rows_table(table_ref, member, level, rank))
            total = term if total is None else total + term
            level += 1
        place += size
    refs[-1][...] = total[:, rank:]
    if last:
        sums = None
        for ref in refs[:count]:
            if ref.shape[0] == half + 8:
                sums = ref[half:] if sums is None else sums + ref[half:]
        refs[count][...] = sums
    else:
        value = keep_ref[...] + got_ref[rank:] + total[:, :rank]
        refs[count][...] = value
        if len(refs) == count + 3:
            refs[count + 1][...] = exact_right(value, upper_ref[1 - member, 0, 0])


def far_rows(mine_ref, theirs_ref):
    mine, theirs = mine_ref[...], theirs_ref[...]
    first = lax.axis_index("leaf") % 2 == 0
    return jnp.concatenate(
        [jnp.where(first, mine, theirs), jnp.where(first, theirs, mine)], axis=0
    ).T


def expand(member, base, far):
    if member == 0:
        return exact_left(base, far)
    return mm(base, far.astype(BF16))


def finish_value(other, rows, leaf, base_refs, u_ref, leaf_far):
    rank = u_ref.shape[-1]
    value = rows_of(base_refs, leaf, rows)
    moved = expand(other, u_ref[leaf], leaf_far[leaf * rank : (leaf + 1) * rank])
    return value + moved if other == 1 else value - moved


def local_kernel(member, first, counts, *refs):
    refs = list(refs)
    near_ref, u_ref, wide_ref, coef_ref, got_ref = (refs.pop(0) for _ in range(5))
    base_refs = tuple(refs.pop(0) for _ in range(counts[0]))
    other_refs = tuple(refs.pop(0) for _ in range(counts[1]))
    other = 1 - member
    leaves, rows, rank = u_ref.shape
    if first:
        coef = coef_ref[...]
        sibling = got_ref[:rank]
    else:
        before_ref, down_ref, feed_ref, sibling_ref, mine_ref, theirs_ref = (
            refs.pop(0) for _ in range(6)
        )
        far = far_rows(mine_ref, theirs_ref)
        coef = coef_ref[...] + left_mul((feed_ref[0, other], feed_ref[1, other]), far)
        sibling = got_ref[:rank] + left_mul((sibling_ref[0, other], sibling_ref[1, other]), far)
        leaf_far = left_mul((down_ref[0, other], down_ref[1, other]), far)
    table = (wide_ref[0, member], wide_ref[1, member])
    inner = left_mul(table, jnp.concatenate([sibling, coef], axis=0))
    norm = None
    for leaf in range(leaves):
        part = slice(leaf * rows, (leaf + 1) * rows)
        small = slice(leaf * rank, (leaf + 1) * rank)
        if first:
            value = rows_of(base_refs, leaf, rows)
        else:
            value = finish_value(other, rows, leaf, base_refs, before_ref, leaf_far)
            if other == 1:
                refs[1][part] = value
            else:
                term = jnp.sum(value * value, axis=0, keepdims=True)
                norm = term if norm is None else norm + term
        near = near_ref[member, leaf]
        if member == 0:
            result = exact_left(near, value)
        else:
            result = mm(near, value.astype(BF16))
        result = result + expand(member, u_ref[leaf], inner[small])
        if member == 0:
            result = rows_of(other_refs, leaf, rows) - result
        elif not first:
            result = rows_of(other_refs, leaf, rows) + result
        refs[0][part] = result
    if norm is not None:
        refs[1][...] = norm


def lift_kernel(other, value_ref, vt_ref, up_ref, next_ref, send_ref, keep_ref):
    leaves, rank, rows = vt_ref.shape
    for leaf in range(leaves):
        value = value_ref[leaf * rows : (leaf + 1) * rows]
        small = slice(leaf * rank, (leaf + 1) * rank)
        if other == 0:
            next_ref[small] = exact_left(vt_ref[leaf], value)
        else:
            next_ref[small] = mm(vt_ref[leaf], value.astype(BF16))
    lifted = left_mul((up_ref[0], up_ref[1]), next_ref[...])
    send_parts(lifted[:rank], lifted[rank:], send_ref, keep_ref)


def last_value_kernel(base_ref, u_ref, down_ref, mine_ref, theirs_ref, *refs):
    *old_refs, value_ref, norm_ref = refs
    leaves, rows, _ = u_ref.shape
    far = far_rows(mine_ref, theirs_ref)
    leaf_far = left_mul((down_ref[0, 0], down_ref[1, 0]), far)
    norm = None
    for leaf in range(leaves):
        value = finish_value(0, rows, leaf, (base_ref,), u_ref, leaf_far)
        value_ref[leaf * rows : (leaf + 1) * rows] = value.astype(BF16)
        term = jnp.sum(value * value, axis=0, keepdims=True)
        norm = term if norm is None else norm + term
    norm_ref[...] = jnp.zeros_like(norm_ref)
    for index, ref in enumerate(old_refs):
        norm_ref[index : index + 1] = ref[...]
    norm_ref[len(old_refs) : len(old_refs) + 1] = norm


def last_local_kernel(near_ref, u_ref, wide_ref, coef_ref, got_ref, *refs):
    value_ref, other_ref, feed_ref, sibling_ref, mine_ref, theirs_ref, out_ref = refs
    leaves, rows, rank = u_ref.shape
    far = far_rows(mine_ref, theirs_ref)
    coef = coef_ref[...] + left_mul((feed_ref[0, 0], feed_ref[1, 0]), far)
    sibling = got_ref[:rank] + left_mul((sibling_ref[0, 0], sibling_ref[1, 0]), far)
    table = (wide_ref[0, 1], wide_ref[1, 1])
    inner = left_mul(table, jnp.concatenate([sibling, coef], axis=0))
    for leaf in range(leaves):
        part = slice(leaf * rows, (leaf + 1) * rows)
        result = mm(near_ref[1, leaf], value_ref[part])
        result = result + expand(1, u_ref[leaf], inner[leaf * rank : (leaf + 1) * rank])
        out_ref[part] = other_ref[part] + result


def finish_kernel(u_ref, down_ref, base_ref, mine_ref, theirs_ref, out_ref):
    leaves, rows, _ = u_ref.shape
    far = far_rows(mine_ref, theirs_ref)
    leaf_far = left_mul((down_ref[0, 1], down_ref[1, 1]), far)
    for leaf in range(leaves):
        value = finish_value(1, rows, leaf, (base_ref,), u_ref, leaf_far)
        out_ref[leaf * rows : (leaf + 1) * rows] = value


def body(right_sides, near_blocks, leaf_bases, local_factors, upper_factors, top_couplings):
    bits_leaf = lax.axis_size("leaf").bit_length() - 1
    bits_rows = lax.axis_size("rows").bit_length() - 1
    devices = lax.axis_size("rows") * lax.axis_size("leaf")
    leaves = near_blocks.shape[1]
    columns = right_sides.shape[1]
    rank = leaf_bases.shape[-1]
    half = columns // 2
    stages = stages_of(bits_leaf + bits_rows)

    def swap(value, mask):
        pairs = [(source, source ^ mask) for source in range(devices)]
        return lax.ppermute(value, ("rows", "leaf"), pairs)

    unit = 2 * rank * rank * columns
    message = ((half, rank), F32)
    lifted = ((rank + half, rank), F32)
    coefs = ((leaves * rank, columns), F32)
    size = (right_sides.shape, F32)
    wide_half = ((right_sides.shape[0] // 2, columns), F32)
    basis = ((leaves, leaf_bases.shape[3], rank), BF16)
    turned = ((leaves, rank, leaf_bases.shape[3]), BF16)
    node = (local_factors.shape[1:], BF16)
    rises = ((2, 2 * rank, leaves * rank), BF16)
    loaded = call(
        functools.partial(start_kernel, leaves),
        [wide_half, wide_half, basis, basis, basis, node, node, turned, rises, coefs, lifted, message],
        [right_sides, leaf_bases, local_factors],
        150 * unit,
        hbm=True,
        scratch=[pltpu.VMEM(*basis), pltpu.SemaphoreType.DMA((8,))],
    )
    right = loaded[:2]
    u = loaded[2:4]
    v_operator, local_operator, local_inverse, vt_inverse, up_inverse = loaded[4:9]
    coef, send, keep = loaded[9:]
    got = swap(send, 1)
    near = near_blocks
    upper = upper_factors[:, 0]

    vt = [None, vt_inverse]
    up = [None, up_inverse]
    stage_tables, plan = [], []
    member = 1
    base = current = right
    chip = chip_risen = None
    norms = []
    mine = theirs = None
    applies = 2 * STEPS + 1
    plan = [1 if len(stage) == 1 else 3 for stage in stages]
    for index in range(applies):
        last = index == applies - 1
        other = 1 - member
        arrived = []
        value, risen = chip, chip_risen
        norm = None
        for number, stage in enumerate(stages):
            low = 2 ** stage[0]
            lower_level = stage[0] - 1
            top_stage = number == len(stages) - 1
            masks = (low,) if len(stage) == 1 else (low, 2 * low, 3 * low)
            sent = [value, risen, risen][: len(masks)]
            if index == 0 and len(stage) > 1:
                tall = message if top_stage else ((half + 2 * rank, rank), F32)
                if number == 0 or not top_stage:
                    sent = call(
                        functools.partial(pack_kernel, lower_level, top_stage),
                        [tall, tall, message],
                        [upper] + ([value] if number else [keep, got]),
                        unit,
                    )
                value = sent[0]
            elif index == 0 and value is None:
                value = keep + got[rank:]
                sent = [value] * len(masks)
            batch = [swap(data, mask) for data, mask in zip(sent, masks)]
            arrived += batch
            if index == 0 and not top_stage:
                stage_tables += call(
                    functools.partial(stage_table_kernel, lower_level, half),
                    [((2, 2, 3 * rank, rank), BF16)],
                    [upper] + batch[:2],
                    16 * unit,
                )
            if number == 0:
                if index == 0:
                    tables = call(
                        functools.partial(local_table_kernel, leaves),
                        [
                            turned,
                            rises,
                            ((2, 2, leaves * rank, (leaves + 1) * rank), BF16),
                            ((2, 2, leaves * rank, rank), BF16),
                            ((2, 2, leaves * rank, rank), BF16),
                            ((4, rank, rank), F32),
                        ],
                        [local_operator, local_inverse] + list(u) + [v_operator, vt_inverse, up_inverse],
                        300 * unit,
                    )
                    vt[0], up[0], wide, down, feed, chip_feed = tables
                    chip_got = swap(chip_feed, 1)
                if last:
                    finished, norm = call(
                        last_value_kernel,
                        [(right_sides.shape, BF16), ((8, columns), F32)],
                        [base, u[0], down, mine, theirs] + norms,
                        100 * unit,
                    )
                    norm_got = swap(norm, 1)
                    base = call(
                        last_local_kernel,
                        [size],
                        [near, u[1], wide, coef, got, finished, current, feed, sibling_table]
                        + [mine, theirs],
                        100 * unit,
                    )[0]
                else:
                    args = [near, u[member], wide, coef, got]
                    base_list = list(base) if isinstance(base, (list, tuple)) else [base]
                    other_list = list(right) if member == 0 else [] if index == 0 else [current]
                    args += base_list + other_list
                    if index:
                        args += [u[other], down, feed, sibling_table, mine, theirs]
                    outs = [size]
                    if index:
                        outs.append(size if member == 0 else ((1, columns), F32))
                    counts = (len(base_list), len(other_list))
                    results = call(
                        functools.partial(local_kernel, member, index == 0, counts),
                        outs,
                        args,
                        200 * unit,
                    )
                    base = results[0]
                    coef, send, next_keep = call(
                        functools.partial(lift_kernel, other),
                        [coefs, lifted, message],
                        [base, vt[other], up[other]],
                        100 * unit,
                    )
                    next_got = swap(send, 1)
                    if index and member == 0:
                        current = results[1]
                    elif index:
                        norms.append(results[1])
            if not top_stage:
                extra = [norm, norm_got] if last and number == len(stages) - 2 else []
                shape = ((half + (8 if extra else 0), rank), F32)
                lift = stages[number + 1][0] - 1 if len(stages[number + 1]) > 1 else None
                results = call(
                    functools.partial(stage_kernel, member, half, lift),
                    [shape] * (1 if lift is None else 2),
                    [upper, stage_tables[number], value] + batch + extra,
                    8 * unit,
                )
                value, risen = results[0], results[-1]
        if index == 0:
            far_table, sibling_table = call(
                far_table_kernel,
                [
                    ((2, 2, (upper.shape[1] + 1) * rank, 2 * rank), BF16),
                    ((2, 2, rank, rank), BF16),
                ],
                [upper, top_couplings, chip_feed, chip_got],
                100 * unit,
            )
        outs = [((8, columns), F32), message]
        if not last:
            outs = [message] * (3 if len(stages[0]) > 1 else 2)
        results = call(
            functools.partial(far_kernel, member, last, plan, half),
            outs,
            [upper, far_table] + ([keep, got] if last else [next_keep, next_got]) + arrived,
            20 * unit,
        )
        chip, chip_risen, mine = results[0], results[-2], results[-1]
        theirs = swap(mine, 1)
        if last:
            sums = chip + value[half:]
        else:
            keep, got = next_keep, next_got
        member = other
    solution = call(finish_kernel, [size], [u[1], down, base, mine, theirs], 30 * unit)[0]
    for stage in stages[:-1]:
        low = 2 ** stage[0]
        masks = (low,) if len(stage) == 1 else (low, 2 * low, 3 * low)
        sums = sum([swap(sums, mask) for mask in masks], sums)
    return solution, sums[:STEPS]


def stages_of(levels_up):
    return [tuple(range(level, min(level + 2, levels_up))) for level in range(1, levels_up, 2)]


def solution(mesh):
    placed = (
        P(("rows", "leaf"), None),
        P(None, ("rows", "leaf"), None, None),
        P(None, ("rows", "leaf"), None, None, None),
        P(None, ("rows", "leaf"), None, None, None),
        P(None, ("rows", "leaf"), None, None, None, None),
        P(),
    )

    return jax.shard_map(
        body,
        mesh=mesh,
        in_specs=placed,
        out_specs=(P(("rows", "leaf"), None), P()),
        check_vma=False,
    )
```

```python
import functools

import jax
import jax.numpy as jnp
from jax import lax
from jax.experimental import pallas as pl
from jax.experimental.pallas import tpu as pltpu
from jax.sharding import PartitionSpec as P


STEPS = 3
CROSSING = (1, 0)
BF16 = jnp.bfloat16
F32 = jnp.float32
VMEM_LIMIT = 16 * 2**20
START_LIMIT = 48 * 2**20


def mm(left, right):
    return jnp.dot(left, right, preferred_element_type=F32)


def pieces(value):
    high = value.astype(BF16)
    return high, (value - high.astype(F32)).astype(BF16)


def left_mul(table, value):
    high, low = pieces(value)
    width = value.shape[1]
    both = mm(table[0], jnp.concatenate([high, low], axis=1))
    return both[:, :width] + both[:, width:] + mm(table[1], high)


def right_mul(value, table):
    high, low = pieces(value)
    rows = value.shape[0]
    both = mm(jnp.concatenate([high, low], axis=0), table[0])
    return both[:rows] + both[rows:] + mm(high, table[1])


def exact_left(table, value):
    high, low = pieces(value)
    width = value.shape[1]
    both = mm(table, jnp.concatenate([high, low], axis=1))
    return both[:, :width] + both[:, width:]


def exact_right(value, table):
    high, low = pieces(value)
    rows = value.shape[0]
    both = mm(jnp.concatenate([high, low], axis=0), table)
    return both[:rows] + both[rows:]


def chain_left(member, table, value):
    return exact_left(table, value) if member == 0 else mm(table, value.astype(BF16))


def chain_right(member, value, table):
    return exact_right(value, table) if member == 0 else mm(value.astype(BF16), table)


def table_left(member, table, value):
    return left_mul(table, value) if member == 0 else mm(table[0], value.astype(BF16))


def table_right(member, value, table):
    return right_mul(value, table) if member == 0 else mm(value.astype(BF16), table[0])


def put(member, ref, index, value):
    high = value.astype(BF16)
    ref[(0,) + index] = high
    if member == 0:
        ref[(1,) + index] = (value - high.astype(F32)).astype(BF16)


def call(kernel, outs, args, flops, hbm=False, scratch=()):
    specs = [pl.BlockSpec(memory_space=pltpu.HBM if hbm else pltpu.VMEM)] * len(args)
    return pl.pallas_call(
        kernel,
        out_shape=[jax.ShapeDtypeStruct(shape, dtype) for shape, dtype in outs],
        in_specs=specs,
        out_specs=[pl.BlockSpec(memory_space=pltpu.VMEM)] * len(outs),
        scratch_shapes=list(scratch),
        compiler_params=pltpu.CompilerParams(vmem_limit_bytes=START_LIMIT if hbm else VMEM_LIMIT),
        cost_estimate=pl.CostEstimate(flops=flops, bytes_accessed=0, transcendentals=0),
    )(*args)


def level_offsets(leaf_count):
    offsets, count, offset = [], leaf_count, 0
    while count >= 1:
        offsets.append(offset)
        offset += count
        count //= 2
    return offsets


def column_half():
    leaf_size = lax.axis_size("leaf")
    device = lax.axis_index("rows") * leaf_size + lax.axis_index("leaf")
    levels_up = (lax.axis_size("rows") * leaf_size).bit_length() - 1
    half = device % 2
    for number, stage in enumerate(stages_of(levels_up)):
        half = half + device // 2 ** stage[crossing_level(number, stage)] % 2
    return half % 2


def crossing_level(number, stage):
    return min(CROSSING[min(number, 1)], len(stage) - 1)


def masks_of(number, stage):
    low = 2 ** stage[0]
    flip = 2 ** stage[crossing_level(number, stage)]
    masks = (low,) if len(stage) == 1 else (low, 2 * low, 3 * low)
    return tuple(mask ^ 1 if mask & flip else mask for mask in masks)


def send_parts(device, lifted, send_ref, keep_ref):
    columns = lifted.shape[1]
    half = columns // 2
    turned = lifted.T
    first = column_half() == 0
    keep_ref[...] = jnp.where(first, turned[:half], turned[half:])
    send_ref[: device.shape[0]] = device
    send_ref[device.shape[0] :] = jnp.where(first, turned[half:], turned[:half])


def start_kernel(leaves, *refs):
    right_hbm, bases_hbm, local_hbm = refs[:3]
    upper_rows_ref, lower_rows_ref, u0_ref, u1_ref, v0_ref, local0_ref, local1_ref = refs[3:10]
    vt_ref, up_ref, coef_ref, send_ref, keep_ref, v1_ref, semaphores = refs[10:]
    rows = right_hbm.shape[0] // leaves
    middle = right_hbm.shape[0] // 2
    copies = [
        pltpu.make_async_copy(source, target, semaphores.at[index])
        for index, (source, target) in enumerate(
            [
                (local_hbm.at[1], local1_ref),
                (bases_hbm.at[1, :, 1], v1_ref),
                (right_hbm.at[:middle], upper_rows_ref),
                (right_hbm.at[middle:], lower_rows_ref),
                (local_hbm.at[0], local0_ref),
                (bases_hbm.at[0, :, 1], v0_ref),
                (bases_hbm.at[1, :, 0], u1_ref),
                (bases_hbm.at[0, :, 0], u0_ref),
            ]
        )
    ]
    for copy in copies:
        copy.start()
    copies[0].wait()
    rank = local1_ref.shape[-1]
    up_table(1, leaves, local1_ref, up_ref)
    copies[1].wait()
    for leaf in range(leaves):
        vt_ref[leaf] = v1_ref[leaf].T
    copies[2].wait()
    copies[3].wait()
    for leaf in range(leaves):
        value = rows_of((upper_rows_ref, lower_rows_ref), leaf, rows).astype(BF16)
        coef_ref[leaf * rank : (leaf + 1) * rank] = mm(vt_ref[leaf], value)
    lifted = mm(up_ref[0], coef_ref[...].astype(BF16))
    send_parts(lifted[:rank], lifted[rank:], send_ref, keep_ref)
    for copy in copies[4:]:
        copy.wait()


def rows_of(refs, leaf, rows):
    held = refs[0].shape[0] // rows
    place = (leaf % held) * rows
    return refs[leaf // held][place : place + rows]


def up_table(member, leaves, local_ref, up_ref):
    rank = local_ref.shape[-1]
    offsets = level_offsets(leaves)
    turned = {}

    def transfer(node):
        if node not in turned:
            turned[node] = local_ref[node, 0].T
        return turned[node]

    for leaf in range(leaves):
        trail = transfer(leaf).astype(F32)
        for depth in range(1, len(offsets)):
            if depth == len(offsets) - 1:
                put(member, up_ref, (slice(0, rank), pl.ds(leaf * rank, rank)), trail)
            trail = chain_left(member, transfer(offsets[depth] + (leaf >> depth)), trail)
        put(member, up_ref, (slice(rank, 2 * rank), pl.ds(leaf * rank, rank)), trail)


def pack_kernel(base, last, upper_ref, *refs):
    near_ref, far_ref, cross_ref = refs[-3:]
    half = cross_ref.shape[0]
    rank = upper_ref.shape[-1]
    value = refs[0][...]
    if len(refs) == 5:
        value = value + refs[1][rank:]
    risen = chain_right(1, value, upper_ref[1, base, 0])
    near_ref[:half] = value
    far_ref[:half] = risen
    cross_ref[...] = risen
    if not last:
        for member in range(2):
            rows = pl.ds(half + member * rank, rank)
            near_ref[rows] = upper_ref[member, base, 0].astype(F32)
            far_ref[rows] = upper_ref[member, base + 1, 0].astype(F32)


def stage_table_kernel(base, half, upper_ref, near_ref, far_ref, out_ref):
    rank = upper_ref.shape[-1]
    for member in range(2):
        rows = pl.ds(half + member * rank, rank)
        here = upper_ref[member, base + 1, 0]
        put(member, out_ref, (member, pl.ds(0, rank)), mm(upper_ref[member, base, 0], here))
        put(member, out_ref, (member, pl.ds(rank, rank)), mm(near_ref[rows].astype(BF16), here))
        put(member, out_ref, (member, pl.ds(2 * rank, rank)), far_ref[rows])


def local_table_kernel(leaves, *refs):
    local_refs, u_refs = refs[0:2], refs[2:4]
    v0_ref, vt1_ref, up1_ref, vt0_ref, up0_ref, wide_ref, down_ref, feed_ref, chip_ref = refs[4:]
    vt_refs, up_refs = (vt0_ref, vt1_ref), (up0_ref, up1_ref)
    rank = up1_ref.shape[-1] // leaves
    offsets = level_offsets(leaves)
    own = offsets[-1]
    up_table(0, leaves, local_refs[0], up0_ref)
    for leaf in range(leaves):
        vt0_ref[leaf] = v0_ref[leaf].T
    for member in (1, 0):
        other = 1 - member
        local_ref = local_refs[member]
        sign = 1.0 if member == 1 else -1.0
        total = None
        turned = {}

        def transfer(node):
            if node not in turned:
                turned[node] = local_ref[node, 0].T
            return turned[node]

        for leaf in range(leaves):
            rows = pl.ds(leaf * rank, rank)
            trail = None
            for depth in range(len(offsets) - 1):
                node = leaf >> depth
                step = local_ref[offsets[depth] + node, 1]
                coupling = local_ref[offsets[depth] + node, 2]
                coupled = (
                    coupling.astype(F32) if trail is None else chain_right(member, trail, coupling)
                )
                for peer in range(leaves):
                    if peer >> depth != node ^ 1:
                        continue
                    entry = coupled
                    for lower in range(depth - 1, -1, -1):
                        entry = chain_right(
                            member, entry, transfer(offsets[lower] + (peer >> lower))
                        )
                    put(member, wide_ref, (member, rows, pl.ds((1 + peer) * rank, rank)), entry)
                trail = step.astype(F32) if trail is None else chain_right(member, trail, step)
            put(
                member,
                wide_ref,
                (member, rows, pl.ds((1 + leaf) * rank, rank)),
                jnp.zeros((rank, rank), F32),
            )
            put(
                member,
                wide_ref,
                (member, rows, pl.ds(0, rank)),
                chain_right(member, trail, local_ref[own, 2]),
            )
            below = chain_right(member, trail, local_ref[own, 1])
            put(member, down_ref, (member, rows), below)
            basis = mm(vt_refs[other][leaf], u_refs[member][leaf])
            feed = (sign * mm(basis.astype(BF16), below.astype(BF16))).astype(BF16)
            feed_ref[member, rows] = feed
            term = mm(up_refs[other][0, :, pl.ds(leaf * rank, rank)], feed)
            total = term if total is None else total + term
        chip_ref[2 * member] = total[:rank]
        chip_ref[2 * member + 1] = total[rank:].T


def far_table_kernel(upper_ref, top_ref, chip_ref, got_ref, far_ref, sibling_ref):
    position = lax.axis_index("rows") // (lax.axis_size("rows") // 2)
    rank = top_ref.shape[-1]
    for member in range(2):
        sibling_ref[member] = got_ref[2 * member].astype(BF16)
        loop = (chip_ref[2 * member + 1] + got_ref[2 * member + 1]).astype(BF16)
        trail = None
        levels = upper_ref.shape[1] + 1
        for level in range(levels):
            if level == levels - 1:
                coupling = jnp.where(position == 0, top_ref[member, 0], top_ref[member, 1])
            else:
                coupling = upper_ref[member, level, 2]
            coupling = coupling.T
            weight = coupling.astype(F32)
            if trail is not None:
                weight = chain_left(member, coupling, trail)
            if level < levels - 1:
                step = upper_ref[member, level, 1].T
                trail = step.astype(F32) if trail is None else chain_left(member, step, trail)
            rows = pl.ds(level * rank, rank)
            put(member, far_ref, (member, rows, slice(0, rank)), chain_right(member, weight, loop))
            put(member, far_ref, (member, rows, slice(rank, 2 * rank)), weight)


def stage_kernel(member, half, lift, upper_ref, table_ref, own_ref, *refs):
    near_ref, far_ref, cross_ref = refs[:3]
    both = far_ref[:half] + cross_ref[:half]
    value = jnp.concatenate([own_ref[:half], near_ref[:half], both], axis=1)
    total = table_right(member, value, (table_ref[0, member], table_ref[1, member]))
    outs = refs[3:]
    if lift is None:
        outs = outs[-1:]
    elif len(outs) > 2:
        outs = outs[-2:]
    outs[0][:half] = total
    if lift is not None:
        outs[1][:half] = chain_right(member, total, upper_ref[member, lift, 0])
    if outs[0].shape[0] > half:
        for ref in outs:
            ref[half:] = refs[3][...] + refs[4][...]


def far_kernel(member, last, plan, half, upper_ref, table_ref, keep_ref, got_ref, *refs):
    rank = table_ref.shape[-1] // 2
    count = sum(plan)
    parts = []
    place = 0
    for size in plan:
        parts.append(refs[place][:half])
        if size == 3:
            parts.append(refs[place + 1][:half] + refs[place + 2][:half])
        place += size
    value = jnp.concatenate(parts, axis=1)
    total = table_right(member, value, (table_ref[0, member], table_ref[1, member]))
    refs[-1][...] = total[:, rank:]
    if last:
        sums = None
        for ref in refs[:count]:
            if ref.shape[0] == half + 8:
                sums = ref[half:] if sums is None else sums + ref[half:]
        refs[count][...] = sums
    else:
        value = keep_ref[...] + got_ref[rank:] + total[:, :rank]
        refs[count][...] = value
        if len(refs) == count + 3:
            refs[count + 1][...] = chain_right(1 - member, value, upper_ref[1 - member, 0, 0])


def far_rows(mine_ref, theirs_ref):
    mine, theirs = mine_ref[...], theirs_ref[...]
    first = column_half() == 0
    return jnp.concatenate(
        [jnp.where(first, mine, theirs), jnp.where(first, theirs, mine)], axis=0
    ).T


def expand(member, base, far):
    if member == 0:
        return exact_left(base, far)
    return mm(base, far.astype(BF16))


def finish_value(other, rows, leaf, base_refs, u_ref, leaf_far):
    rank = u_ref.shape[-1]
    value = rows_of(base_refs, leaf, rows)
    moved = expand(other, u_ref[leaf], leaf_far[leaf * rank : (leaf + 1) * rank])
    return value + moved if other == 1 else value - moved


def local_kernel(member, first, counts, *refs):
    refs = list(refs)
    near_ref, u_ref, wide_ref, coef_ref, got_ref = (refs.pop(0) for _ in range(5))
    base_refs = tuple(refs.pop(0) for _ in range(counts[0]))
    other_refs = tuple(refs.pop(0) for _ in range(counts[1]))
    other = 1 - member
    leaves, rows, rank = u_ref.shape
    if first:
        coef = coef_ref[...]
        sibling = got_ref[:rank]
    else:
        before_ref, down_ref, feed_ref, sibling_ref, mine_ref, theirs_ref = (
            refs.pop(0) for _ in range(6)
        )
        far = far_rows(mine_ref, theirs_ref)
        rounded = far.astype(BF16)
        coef = coef_ref[...] + mm(feed_ref[other], rounded)
        sibling = got_ref[:rank] + mm(sibling_ref[other], rounded)
        leaf_far = table_left(other, (down_ref[0, other], down_ref[1, other]), far)
    table = (wide_ref[0, member], wide_ref[1, member])
    inner = table_left(member, table, jnp.concatenate([sibling, coef], axis=0))
    norm = None
    for leaf in range(leaves):
        part = slice(leaf * rows, (leaf + 1) * rows)
        small = slice(leaf * rank, (leaf + 1) * rank)
        if first:
            value = rows_of(base_refs, leaf, rows)
        else:
            value = finish_value(other, rows, leaf, base_refs, before_ref, leaf_far)
            if other == 1:
                refs[1][part] = value
            else:
                term = jnp.sum(value * value, axis=0, keepdims=True)
                norm = term if norm is None else norm + term
        near = near_ref[member, leaf]
        if member == 0:
            result = exact_left(near, value)
        else:
            result = mm(near, value.astype(BF16))
        result = result + expand(member, u_ref[leaf], inner[small])
        if member == 0:
            result = rows_of(other_refs, leaf, rows) - result
        elif not first:
            result = rows_of(other_refs, leaf, rows) + result
        refs[0][part] = result
    if norm is not None:
        refs[1][...] = norm


def lift_kernel(other, value_ref, vt_ref, up_ref, next_ref, send_ref, keep_ref):
    leaves, rank, rows = vt_ref.shape
    for leaf in range(leaves):
        value = value_ref[leaf * rows : (leaf + 1) * rows]
        small = slice(leaf * rank, (leaf + 1) * rank)
        if other == 0:
            next_ref[small] = exact_left(vt_ref[leaf], value)
        else:
            next_ref[small] = mm(vt_ref[leaf], value.astype(BF16))
    lifted = table_left(other, (up_ref[0], up_ref[1]), next_ref[...])
    send_parts(lifted[:rank], lifted[rank:], send_ref, keep_ref)


def last_value_kernel(base_ref, u_ref, down_ref, mine_ref, theirs_ref, *refs):
    *old_refs, value_ref, norm_ref = refs
    leaves, rows, _ = u_ref.shape
    far = far_rows(mine_ref, theirs_ref)
    leaf_far = left_mul((down_ref[0, 0], down_ref[1, 0]), far)
    norm = None
    for leaf in range(leaves):
        value = finish_value(0, rows, leaf, (base_ref,), u_ref, leaf_far)
        value_ref[leaf * rows : (leaf + 1) * rows] = value.astype(BF16)
        term = jnp.sum(value * value, axis=0, keepdims=True)
        norm = term if norm is None else norm + term
    norm_ref[...] = jnp.zeros_like(norm_ref)
    for index, ref in enumerate(old_refs):
        norm_ref[index : index + 1] = ref[...]
    norm_ref[len(old_refs) : len(old_refs) + 1] = norm


def last_local_kernel(near_ref, u_ref, wide_ref, coef_ref, got_ref, *refs):
    value_ref, other_ref, feed_ref, sibling_ref, mine_ref, theirs_ref, out_ref = refs
    leaves, rows, rank = u_ref.shape
    far = far_rows(mine_ref, theirs_ref)
    rounded = far.astype(BF16)
    coef = coef_ref[...] + mm(feed_ref[0], rounded)
    sibling = got_ref[:rank] + mm(sibling_ref[0], rounded)
    table = (wide_ref[0, 1], wide_ref[1, 1])
    inner = table_left(1, table, jnp.concatenate([sibling, coef], axis=0))
    for leaf in range(leaves):
        part = slice(leaf * rows, (leaf + 1) * rows)
        result = mm(near_ref[1, leaf], value_ref[part])
        result = result + expand(1, u_ref[leaf], inner[leaf * rank : (leaf + 1) * rank])
        out_ref[part] = other_ref[part] + result


def finish_kernel(u_ref, down_ref, base_ref, mine_ref, theirs_ref, out_ref):
    leaves, rows, _ = u_ref.shape
    far = far_rows(mine_ref, theirs_ref)
    leaf_far = table_left(1, (down_ref[0, 1], down_ref[1, 1]), far)
    for leaf in range(leaves):
        value = finish_value(1, rows, leaf, (base_ref,), u_ref, leaf_far)
        out_ref[leaf * rows : (leaf + 1) * rows] = value


def body(right_sides, near_blocks, leaf_bases, local_factors, upper_factors, top_couplings):
    bits_leaf = lax.axis_size("leaf").bit_length() - 1
    bits_rows = lax.axis_size("rows").bit_length() - 1
    devices = lax.axis_size("rows") * lax.axis_size("leaf")
    leaves = near_blocks.shape[1]
    columns = right_sides.shape[1]
    rank = leaf_bases.shape[-1]
    half = columns // 2
    stages = stages_of(bits_leaf + bits_rows)

    def swap(value, mask):
        pairs = [(source, source ^ mask) for source in range(devices)]
        return lax.ppermute(value, ("rows", "leaf"), pairs)

    unit = 2 * rank * rank * columns
    message = ((half, rank), F32)
    lifted = ((rank + half, rank), F32)
    coefs = ((leaves * rank, columns), F32)
    size = (right_sides.shape, F32)
    wide_half = ((right_sides.shape[0] // 2, columns), F32)
    basis = ((leaves, leaf_bases.shape[3], rank), BF16)
    turned = ((leaves, rank, leaf_bases.shape[3]), BF16)
    node = (local_factors.shape[1:], BF16)
    rises = ((2, 2 * rank, leaves * rank), BF16)
    loaded = call(
        functools.partial(start_kernel, leaves),
        [wide_half, wide_half, basis, basis, basis, node, node, turned, rises, coefs, lifted, message],
        [right_sides, leaf_bases, local_factors],
        150 * unit,
        hbm=True,
        scratch=[pltpu.VMEM(*basis), pltpu.SemaphoreType.DMA((8,))],
    )
    right = loaded[:2]
    u = loaded[2:4]
    v_operator, local_operator, local_inverse, vt_inverse, up_inverse = loaded[4:9]
    coef, send, keep = loaded[9:]
    got = swap(send, 1)
    near = near_blocks
    upper = upper_factors[:, 0]

    vt = [None, vt_inverse]
    up = [None, up_inverse]
    stage_tables, plan = [], []
    member = 1
    base = current = right
    chip = chip_risen = None
    norms = []
    mine = theirs = None
    applies = 2 * STEPS + 1
    plan = [1 if len(stage) == 1 else 3 for stage in stages]
    for index in range(applies):
        last = index == applies - 1
        other = 1 - member
        arrived = []
        value, risen = chip, chip_risen
        norm = None
        for number, stage in enumerate(stages):
            lower_level = stage[0] - 1
            top_stage = number == len(stages) - 1
            masks = masks_of(number, stage)
            sent = [value, risen, risen][: len(masks)]
            if index == 0 and len(stage) > 1:
                tall = message if top_stage else ((half + 2 * rank, rank), F32)
                if number == 0 or not top_stage:
                    sent = call(
                        functools.partial(pack_kernel, lower_level, top_stage),
                        [tall, tall, message],
                        [upper] + ([value] if number else [keep, got]),
                        unit,
                    )
                value = sent[0]
            elif index == 0 and value is None:
                value = keep + got[rank:]
                sent = [value] * len(masks)
            batch = [swap(data, mask) for data, mask in zip(sent, masks)]
            arrived += batch
            if index == 0 and not top_stage:
                stage_tables += call(
                    functools.partial(stage_table_kernel, lower_level, half),
                    [((2, 2, 3 * rank, rank), BF16)],
                    [upper] + batch[:2],
                    16 * unit,
                )
            if number == 0:
                if index == 0:
                    tables = call(
                        functools.partial(local_table_kernel, leaves),
                        [
                            turned,
                            rises,
                            ((2, 2, leaves * rank, (leaves + 1) * rank), BF16),
                            ((2, 2, leaves * rank, rank), BF16),
                            ((2, leaves * rank, rank), BF16),
                            ((4, rank, rank), F32),
                        ],
                        [local_operator, local_inverse] + list(u) + [v_operator, vt_inverse, up_inverse],
                        300 * unit,
                    )
                    vt[0], up[0], wide, down, feed, chip_feed = tables
                    chip_got = swap(chip_feed, 1)
                if last:
                    finished, norm = call(
                        last_value_kernel,
                        [(right_sides.shape, BF16), ((8, columns), F32)],
                        [base, u[0], down, mine, theirs] + norms,
                        100 * unit,
                    )
                    norm_got = swap(norm, 1)
                    base = call(
                        last_local_kernel,
                        [size],
                        [near, u[1], wide, coef, got, finished, current, feed, sibling_table]
                        + [mine, theirs],
                        100 * unit,
                    )[0]
                else:
                    args = [near, u[member], wide, coef, got]
                    base_list = list(base) if isinstance(base, (list, tuple)) else [base]
                    other_list = list(right) if member == 0 else [] if index == 0 else [current]
                    args += base_list + other_list
                    if index:
                        args += [u[other], down, feed, sibling_table, mine, theirs]
                    outs = [size]
                    if index:
                        outs.append(size if member == 0 else ((1, columns), F32))
                    counts = (len(base_list), len(other_list))
                    results = call(
                        functools.partial(local_kernel, member, index == 0, counts),
                        outs,
                        args,
                        200 * unit,
                    )
                    base = results[0]
                    coef, send, next_keep = call(
                        functools.partial(lift_kernel, other),
                        [coefs, lifted, message],
                        [base, vt[other], up[other]],
                        100 * unit,
                    )
                    next_got = swap(send, 1)
                    if index and member == 0:
                        current = results[1]
                    elif index:
                        norms.append(results[1])
            if not top_stage:
                extra = [norm, norm_got] if last and number == len(stages) - 2 else []
                shape = ((half + (8 if extra else 0), rank), F32)
                lift = stages[number + 1][0] - 1 if len(stages[number + 1]) > 1 else None
                results = call(
                    functools.partial(stage_kernel, member, half, lift),
                    [shape] * (1 if lift is None else 2),
                    [upper, stage_tables[number], value] + batch + extra,
                    8 * unit,
                )
                value, risen = results[0], results[-1]
        if index == 0:
            far_table, sibling_table = call(
                far_table_kernel,
                [
                    ((2, 2, (upper.shape[1] + 1) * rank, 2 * rank), BF16),
                    ((2, rank, rank), BF16),
                ],
                [upper, top_couplings, chip_feed, chip_got],
                100 * unit,
            )
        outs = [((8, columns), F32), message]
        if not last:
            outs = [message] * (3 if len(stages[0]) > 1 else 2)
        results = call(
            functools.partial(far_kernel, member, last, plan, half),
            outs,
            [upper, far_table] + ([keep, got] if last else [next_keep, next_got]) + arrived,
            20 * unit,
        )
        chip, chip_risen, mine = results[0], results[-2], results[-1]
        theirs = swap(mine, 1)
        if last:
            sums = chip + value[half:]
        else:
            keep, got = next_keep, next_got
        member = other
    solution = call(finish_kernel, [size], [u[1], down, base, mine, theirs], 30 * unit)[0]
    for number, stage in enumerate(stages[:-1]):
        masks = masks_of(number, stage)
        sums = sum([swap(sums, mask) for mask in masks], sums)
    return solution, sums[:STEPS]


def stages_of(levels_up):
    return [tuple(range(level, min(level + 2, levels_up))) for level in range(1, levels_up, 2)]


def solution(mesh):
    placed = (
        P(("rows", "leaf"), None),
        P(None, ("rows", "leaf"), None, None),
        P(None, ("rows", "leaf"), None, None, None),
        P(None, ("rows", "leaf"), None, None, None),
        P(None, ("rows", "leaf"), None, None, None, None),
        P(),
    )

    return jax.shard_map(
        body,
        mesh=mesh,
        in_specs=placed,
        out_specs=(P(("rows", "leaf"), None), P()),
        check_vma=False,
    )
```

```python
import functools

import jax
import jax.numpy as jnp
from jax import lax
from jax.experimental import pallas as pl
from jax.experimental.pallas import tpu as pltpu
from jax.sharding import PartitionSpec as P


STEPS = 3
CROSSING = (1, 0)
BF16 = jnp.bfloat16
F32 = jnp.float32
VMEM_LIMIT = 16 * 2**20
START_LIMIT = 48 * 2**20


def mm(left, right):
    return jnp.dot(left, right, preferred_element_type=F32)


def pieces(value):
    high = value.astype(BF16)
    return high, (value - high.astype(F32)).astype(BF16)


def left_mul(table, value):
    high, low = pieces(value)
    width = value.shape[1]
    both = mm(table[0], jnp.concatenate([high, low], axis=1))
    return both[:, :width] + both[:, width:] + mm(table[1], high)


def right_mul(value, table):
    high, low = pieces(value)
    rows = value.shape[0]
    both = mm(jnp.concatenate([high, low], axis=0), table[0])
    return both[:rows] + both[rows:] + mm(high, table[1])


def exact_left(table, value):
    high, low = pieces(value)
    width = value.shape[1]
    both = mm(table, jnp.concatenate([high, low], axis=1))
    return both[:, :width] + both[:, width:]


def exact_right(value, table):
    high, low = pieces(value)
    rows = value.shape[0]
    both = mm(jnp.concatenate([high, low], axis=0), table)
    return both[:rows] + both[rows:]


def chain_left(member, table, value):
    return exact_left(table, value) if member == 0 else mm(table, value.astype(BF16))


def chain_right(member, value, table):
    return exact_right(value, table) if member == 0 else mm(value.astype(BF16), table)


def table_left(member, table, value):
    return left_mul(table, value) if member == 0 else mm(table[0], value.astype(BF16))


def table_right(member, value, table):
    return right_mul(value, table) if member == 0 else mm(value.astype(BF16), table[0])


def put(member, ref, index, value):
    high = value.astype(BF16)
    ref[(0,) + index] = high
    if member == 0:
        ref[(1,) + index] = (value - high.astype(F32)).astype(BF16)


def call(kernel, outs, args, flops, hbm=False, scratch=()):
    specs = [pl.BlockSpec(memory_space=pltpu.HBM if hbm else pltpu.VMEM)] * len(args)
    return pl.pallas_call(
        kernel,
        out_shape=[jax.ShapeDtypeStruct(shape, dtype) for shape, dtype in outs],
        in_specs=specs,
        out_specs=[pl.BlockSpec(memory_space=pltpu.VMEM)] * len(outs),
        scratch_shapes=list(scratch),
        compiler_params=pltpu.CompilerParams(vmem_limit_bytes=START_LIMIT if hbm else VMEM_LIMIT),
        cost_estimate=pl.CostEstimate(flops=flops, bytes_accessed=0, transcendentals=0),
    )(*args)


def level_offsets(leaf_count):
    offsets, count, offset = [], leaf_count, 0
    while count >= 1:
        offsets.append(offset)
        offset += count
        count //= 2
    return offsets


def column_half():
    leaf_size = lax.axis_size("leaf")
    device = lax.axis_index("rows") * leaf_size + lax.axis_index("leaf")
    levels_up = (lax.axis_size("rows") * leaf_size).bit_length() - 1
    half = device % 2
    for number, stage in enumerate(stages_of(levels_up)):
        half = half + device // 2 ** stage[crossing_level(number, stage)] % 2
    return half % 2


def crossing_level(number, stage):
    return min(CROSSING[min(number, 1)], len(stage) - 1)


def masks_of(number, stage):
    low = 2 ** stage[0]
    flip = 2 ** stage[crossing_level(number, stage)]
    masks = (low,) if len(stage) == 1 else (low, 2 * low, 3 * low)
    return tuple(mask ^ 1 if mask & flip else mask for mask in masks)


def send_parts(device, lifted, send_ref, keep_ref):
    columns = lifted.shape[1]
    half = columns // 2
    turned = lifted.T
    first = column_half() == 0
    keep_ref[...] = jnp.where(first, turned[:half], turned[half:])
    send_ref[: device.shape[0]] = device
    send_ref[device.shape[0] :] = jnp.where(first, turned[half:], turned[:half])


def start_kernel(leaves, *refs):
    right_hbm, bases_hbm, local_hbm = refs[:3]
    upper_rows_ref, lower_rows_ref, u0_ref, u1_ref, v0_ref, local0_ref, local1_ref = refs[3:10]
    vt_ref, up_ref, coef_ref, send_ref, keep_ref, v1_ref, semaphores = refs[10:]
    rows = right_hbm.shape[0] // leaves
    middle = right_hbm.shape[0] // 2
    copies = [
        pltpu.make_async_copy(source, target, semaphores.at[index])
        for index, (source, target) in enumerate(
            [
                (local_hbm.at[1], local1_ref),
                (bases_hbm.at[1, :, 1], v1_ref),
                (right_hbm.at[:middle], upper_rows_ref),
                (right_hbm.at[middle:], lower_rows_ref),
                (local_hbm.at[0], local0_ref),
                (bases_hbm.at[0, :, 1], v0_ref),
                (bases_hbm.at[1, :, 0], u1_ref),
                (bases_hbm.at[0, :, 0], u0_ref),
            ]
        )
    ]
    for copy in copies:
        copy.start()
    copies[0].wait()
    rank = local1_ref.shape[-1]
    up_table(1, leaves, local1_ref, up_ref)
    copies[1].wait()
    for leaf in range(leaves):
        vt_ref[leaf] = v1_ref[leaf].T
    copies[2].wait()
    copies[3].wait()
    for leaf in range(leaves):
        value = rows_of((upper_rows_ref, lower_rows_ref), leaf, rows).astype(BF16)
        coef_ref[leaf * rank : (leaf + 1) * rank] = mm(vt_ref[leaf], value)
    lifted = mm(up_ref[0], coef_ref[...].astype(BF16))
    send_parts(lifted[:rank], lifted[rank:], send_ref, keep_ref)
    for copy in copies[4:]:
        copy.wait()


def rows_of(refs, leaf, rows):
    held = refs[0].shape[0] // rows
    place = (leaf % held) * rows
    return refs[leaf // held][place : place + rows]


def up_table(member, leaves, local_ref, up_ref):
    rank = local_ref.shape[-1]
    offsets = level_offsets(leaves)
    turned = {}

    def transfer(node):
        if node not in turned:
            turned[node] = local_ref[node, 0].T
        return turned[node]

    for leaf in range(leaves):
        trail = transfer(leaf).astype(F32)
        for depth in range(1, len(offsets)):
            if depth == len(offsets) - 1:
                put(member, up_ref, (slice(0, rank), pl.ds(leaf * rank, rank)), trail)
            trail = chain_left(member, transfer(offsets[depth] + (leaf >> depth)), trail)
        put(member, up_ref, (slice(rank, 2 * rank), pl.ds(leaf * rank, rank)), trail)


def pack_kernel(base, last, upper_ref, *refs):
    near_ref, far_ref, cross_ref = refs[-3:]
    half = cross_ref.shape[0]
    rank = upper_ref.shape[-1]
    value = refs[0][...]
    if len(refs) == 5:
        value = value + refs[1][rank:]
    risen = chain_right(1, value, upper_ref[1, base, 0])
    near_ref[:half] = value
    far_ref[:half] = risen
    cross_ref[...] = risen
    if not last:
        for member in range(2):
            rows = pl.ds(half + member * rank, rank)
            near_ref[rows] = upper_ref[member, base, 0].astype(F32)
            far_ref[rows] = upper_ref[member, base + 1, 0].astype(F32)


def stage_table_kernel(base, half, upper_ref, near_ref, far_ref, out_ref):
    rank = upper_ref.shape[-1]
    for member in range(2):
        rows = pl.ds(half + member * rank, rank)
        here = upper_ref[member, base + 1, 0]
        put(member, out_ref, (member, pl.ds(0, rank)), mm(upper_ref[member, base, 0], here))
        put(member, out_ref, (member, pl.ds(rank, rank)), mm(near_ref[rows].astype(BF16), here))
        put(member, out_ref, (member, pl.ds(2 * rank, rank)), far_ref[rows])


def local_table_kernel(leaves, *refs):
    local_refs, u_refs = refs[0:2], refs[2:4]
    v0_ref, vt1_ref, up1_ref, vt0_ref, up0_ref, wide_ref, down_ref, feed_ref, chip_ref = refs[4:]
    vt_refs, up_refs = (vt0_ref, vt1_ref), (up0_ref, up1_ref)
    rank = up1_ref.shape[-1] // leaves
    offsets = level_offsets(leaves)
    own = offsets[-1]
    up_table(0, leaves, local_refs[0], up0_ref)
    for leaf in range(leaves):
        vt0_ref[leaf] = v0_ref[leaf].T
    for member in (1, 0):
        other = 1 - member
        local_ref = local_refs[member]
        sign = 1.0 if member == 1 else -1.0
        total = None
        turned = {}

        def transfer(node):
            if node not in turned:
                turned[node] = local_ref[node, 0].T
            return turned[node]

        for leaf in range(leaves):
            rows = pl.ds(leaf * rank, rank)
            trail = None
            for depth in range(len(offsets) - 1):
                node = leaf >> depth
                step = local_ref[offsets[depth] + node, 1]
                coupling = local_ref[offsets[depth] + node, 2]
                coupled = (
                    coupling.astype(F32) if trail is None else chain_right(member, trail, coupling)
                )
                for peer in range(leaves):
                    if peer >> depth != node ^ 1:
                        continue
                    entry = coupled
                    for lower in range(depth - 1, -1, -1):
                        entry = chain_right(
                            member, entry, transfer(offsets[lower] + (peer >> lower))
                        )
                    put(member, wide_ref, (member, rows, pl.ds((1 + peer) * rank, rank)), entry)
                trail = step.astype(F32) if trail is None else chain_right(member, trail, step)
            put(
                member,
                wide_ref,
                (member, rows, pl.ds((1 + leaf) * rank, rank)),
                jnp.zeros((rank, rank), F32),
            )
            put(
                member,
                wide_ref,
                (member, rows, pl.ds(0, rank)),
                chain_right(member, trail, local_ref[own, 2]),
            )
            below = chain_right(member, trail, local_ref[own, 1])
            put(member, down_ref, (member, rows), below)
            basis = mm(vt_refs[other][leaf], u_refs[member][leaf])
            feed = (sign * mm(basis.astype(BF16), below.astype(BF16))).astype(BF16)
            feed_ref[member, rows] = feed
            term = mm(up_refs[other][0, :, pl.ds(leaf * rank, rank)], feed)
            total = term if total is None else total + term
        chip_ref[2 * member] = total[:rank]
        chip_ref[2 * member + 1] = total[rank:].T


def far_table_kernel(upper_ref, top_ref, chip_ref, got_ref, far_ref, sibling_ref):
    position = lax.axis_index("rows") // (lax.axis_size("rows") // 2)
    rank = top_ref.shape[-1]
    for member in range(2):
        sibling_ref[member] = got_ref[2 * member].astype(BF16)
        loop = (chip_ref[2 * member + 1] + got_ref[2 * member + 1]).astype(BF16)
        trail = None
        levels = upper_ref.shape[1] + 1
        for level in range(levels):
            if level == levels - 1:
                coupling = jnp.where(position == 0, top_ref[member, 0], top_ref[member, 1])
            else:
                coupling = upper_ref[member, level, 2]
            coupling = coupling.T
            weight = coupling.astype(F32)
            if trail is not None:
                weight = chain_left(member, coupling, trail)
            if level < levels - 1:
                step = upper_ref[member, level, 1].T
                trail = step.astype(F32) if trail is None else chain_left(member, step, trail)
            rows = pl.ds(level * rank, rank)
            put(member, far_ref, (member, rows, slice(0, rank)), chain_right(member, weight, loop))
            put(member, far_ref, (member, rows, slice(rank, 2 * rank)), weight)


def stage_kernel(member, half, lift, upper_ref, table_ref, own_ref, *refs):
    near_ref, far_ref, cross_ref = refs[:3]
    both = far_ref[:half] + cross_ref[:half]
    value = jnp.concatenate([own_ref[:half], near_ref[:half], both], axis=1)
    total = table_right(member, value, (table_ref[0, member], table_ref[1, member]))
    outs = refs[3:]
    if lift is None:
        outs = outs[-1:]
    elif len(outs) > 2:
        outs = outs[-2:]
    outs[0][:half] = total
    if lift is not None:
        outs[1][:half] = chain_right(member, total, upper_ref[member, lift, 0])
    if outs[0].shape[0] > half:
        for ref in outs:
            ref[half:] = refs[3][...] + refs[4][...]


def far_kernel(member, last, plan, half, upper_ref, table_ref, keep_ref, got_ref, *refs):
    rank = table_ref.shape[-1] // 2
    count = sum(plan)
    parts = []
    place = 0
    for size in plan:
        parts.append(refs[place][:half])
        if size == 3:
            parts.append(refs[place + 1][:half] + refs[place + 2][:half])
        place += size
    value = jnp.concatenate(parts, axis=1)
    table = (table_ref[0, member, :, rank:], table_ref[1, member, :, rank:])
    feed = mm(value.astype(BF16), table_ref[0, member, :, :rank])
    refs[-1][...] = table_right(member, value, table)
    if last:
        sums = None
        for ref in refs[:count]:
            if ref.shape[0] == half + 8:
                sums = ref[half:] if sums is None else sums + ref[half:]
        refs[count][...] = sums
    else:
        value = keep_ref[...] + got_ref[rank:] + feed
        refs[count][...] = value
        if len(refs) == count + 3:
            refs[count + 1][...] = chain_right(1 - member, value, upper_ref[1 - member, 0, 0])


def far_rows(mine_ref, theirs_ref):
    mine, theirs = mine_ref[...], theirs_ref[...]
    first = column_half() == 0
    return jnp.concatenate(
        [jnp.where(first, mine, theirs), jnp.where(first, theirs, mine)], axis=0
    ).T


def expand(member, base, far):
    if member == 0:
        return exact_left(base, far)
    return mm(base, far.astype(BF16))


def finish_value(other, rows, leaf, base_refs, u_ref, leaf_far):
    rank = u_ref.shape[-1]
    value = rows_of(base_refs, leaf, rows)
    moved = expand(other, u_ref[leaf], leaf_far[leaf * rank : (leaf + 1) * rank])
    return value + moved if other == 1 else value - moved


def local_kernel(member, first, counts, *refs):
    refs = list(refs)
    near_ref, u_ref, wide_ref, coef_ref, got_ref = (refs.pop(0) for _ in range(5))
    base_refs = tuple(refs.pop(0) for _ in range(counts[0]))
    other_refs = tuple(refs.pop(0) for _ in range(counts[1]))
    other = 1 - member
    leaves, rows, rank = u_ref.shape
    if first:
        coef = coef_ref[...]
        sibling = got_ref[:rank]
    else:
        before_ref, down_ref, feed_ref, sibling_ref, mine_ref, theirs_ref = (
            refs.pop(0) for _ in range(6)
        )
        far = far_rows(mine_ref, theirs_ref)
        rounded = far.astype(BF16)
        coef = coef_ref[...] + mm(feed_ref[other], rounded)
        sibling = got_ref[:rank] + mm(sibling_ref[other], rounded)
        leaf_far = table_left(other, (down_ref[0, other], down_ref[1, other]), far)
    table = (wide_ref[0, member], wide_ref[1, member])
    inner = table_left(member, table, jnp.concatenate([sibling, coef], axis=0))
    norm = None
    for leaf in range(leaves):
        part = slice(leaf * rows, (leaf + 1) * rows)
        small = slice(leaf * rank, (leaf + 1) * rank)
        if first:
            value = rows_of(base_refs, leaf, rows)
        else:
            value = finish_value(other, rows, leaf, base_refs, before_ref, leaf_far)
            if other == 1:
                refs[1][part] = value
            else:
                term = jnp.sum(value * value, axis=0, keepdims=True)
                norm = term if norm is None else norm + term
        near = near_ref[member, leaf]
        if member == 0:
            result = exact_left(near, value)
        else:
            result = mm(near, value.astype(BF16))
        result = result + expand(member, u_ref[leaf], inner[small])
        if member == 0:
            result = rows_of(other_refs, leaf, rows) - result
        elif not first:
            result = rows_of(other_refs, leaf, rows) + result
        refs[0][part] = result
    if norm is not None:
        refs[1][...] = norm


def lift_kernel(other, value_ref, vt_ref, up_ref, next_ref, send_ref, keep_ref):
    leaves, rank, rows = vt_ref.shape
    for leaf in range(leaves):
        value = value_ref[leaf * rows : (leaf + 1) * rows]
        small = slice(leaf * rank, (leaf + 1) * rank)
        if other == 0:
            next_ref[small] = exact_left(vt_ref[leaf], value)
        else:
            next_ref[small] = mm(vt_ref[leaf], value.astype(BF16))
    lifted = table_left(other, (up_ref[0], up_ref[1]), next_ref[...])
    send_parts(lifted[:rank], lifted[rank:], send_ref, keep_ref)


def last_value_kernel(base_ref, u_ref, down_ref, mine_ref, theirs_ref, *refs):
    *old_refs, value_ref, norm_ref = refs
    leaves, rows, _ = u_ref.shape
    far = far_rows(mine_ref, theirs_ref)
    leaf_far = left_mul((down_ref[0, 0], down_ref[1, 0]), far)
    norm = None
    for leaf in range(leaves):
        value = finish_value(0, rows, leaf, (base_ref,), u_ref, leaf_far)
        value_ref[leaf * rows : (leaf + 1) * rows] = value.astype(BF16)
        term = jnp.sum(value * value, axis=0, keepdims=True)
        norm = term if norm is None else norm + term
    norm_ref[...] = jnp.zeros_like(norm_ref)
    for index, ref in enumerate(old_refs):
        norm_ref[index : index + 1] = ref[...]
    norm_ref[len(old_refs) : len(old_refs) + 1] = norm


def last_local_kernel(near_ref, u_ref, wide_ref, coef_ref, got_ref, *refs):
    value_ref, other_ref, feed_ref, sibling_ref, mine_ref, theirs_ref, out_ref = refs
    leaves, rows, rank = u_ref.shape
    far = far_rows(mine_ref, theirs_ref)
    rounded = far.astype(BF16)
    coef = coef_ref[...] + mm(feed_ref[0], rounded)
    sibling = got_ref[:rank] + mm(sibling_ref[0], rounded)
    table = (wide_ref[0, 1], wide_ref[1, 1])
    inner = table_left(1, table, jnp.concatenate([sibling, coef], axis=0))
    for leaf in range(leaves):
        part = slice(leaf * rows, (leaf + 1) * rows)
        result = mm(near_ref[1, leaf], value_ref[part])
        result = result + expand(1, u_ref[leaf], inner[leaf * rank : (leaf + 1) * rank])
        out_ref[part] = other_ref[part] + result


def finish_kernel(u_ref, down_ref, base_ref, mine_ref, theirs_ref, out_ref):
    leaves, rows, _ = u_ref.shape
    far = far_rows(mine_ref, theirs_ref)
    leaf_far = table_left(1, (down_ref[0, 1], down_ref[1, 1]), far)
    for leaf in range(leaves):
        value = finish_value(1, rows, leaf, (base_ref,), u_ref, leaf_far)
        out_ref[leaf * rows : (leaf + 1) * rows] = value


def body(right_sides, near_blocks, leaf_bases, local_factors, upper_factors, top_couplings):
    bits_leaf = lax.axis_size("leaf").bit_length() - 1
    bits_rows = lax.axis_size("rows").bit_length() - 1
    devices = lax.axis_size("rows") * lax.axis_size("leaf")
    leaves = near_blocks.shape[1]
    columns = right_sides.shape[1]
    rank = leaf_bases.shape[-1]
    half = columns // 2
    stages = stages_of(bits_leaf + bits_rows)

    def swap(value, mask):
        pairs = [(source, source ^ mask) for source in range(devices)]
        return lax.ppermute(value, ("rows", "leaf"), pairs)

    unit = 2 * rank * rank * columns
    message = ((half, rank), F32)
    lifted = ((rank + half, rank), F32)
    coefs = ((leaves * rank, columns), F32)
    size = (right_sides.shape, F32)
    wide_half = ((right_sides.shape[0] // 2, columns), F32)
    basis = ((leaves, leaf_bases.shape[3], rank), BF16)
    turned = ((leaves, rank, leaf_bases.shape[3]), BF16)
    node = (local_factors.shape[1:], BF16)
    rises = ((2, 2 * rank, leaves * rank), BF16)
    loaded = call(
        functools.partial(start_kernel, leaves),
        [wide_half, wide_half, basis, basis, basis, node, node, turned, rises, coefs, lifted, message],
        [right_sides, leaf_bases, local_factors],
        150 * unit,
        hbm=True,
        scratch=[pltpu.VMEM(*basis), pltpu.SemaphoreType.DMA((8,))],
    )
    right = loaded[:2]
    u = loaded[2:4]
    v_operator, local_operator, local_inverse, vt_inverse, up_inverse = loaded[4:9]
    coef, send, keep = loaded[9:]
    got = swap(send, 1)
    near = near_blocks
    upper = upper_factors[:, 0]

    vt = [None, vt_inverse]
    up = [None, up_inverse]
    stage_tables, plan = [], []
    member = 1
    base = current = right
    chip = chip_risen = None
    norms = []
    mine = theirs = None
    applies = 2 * STEPS + 1
    plan = [1 if len(stage) == 1 else 3 for stage in stages]
    for index in range(applies):
        last = index == applies - 1
        other = 1 - member
        arrived = []
        value, risen = chip, chip_risen
        norm = None
        for number, stage in enumerate(stages):
            lower_level = stage[0] - 1
            top_stage = number == len(stages) - 1
            masks = masks_of(number, stage)
            sent = [value, risen, risen][: len(masks)]
            if index == 0 and len(stage) > 1:
                tall = message if top_stage else ((half + 2 * rank, rank), F32)
                if number == 0 or not top_stage:
                    sent = call(
                        functools.partial(pack_kernel, lower_level, top_stage),
                        [tall, tall, message],
                        [upper] + ([value] if number else [keep, got]),
                        unit,
                    )
                value = sent[0]
            elif index == 0 and value is None:
                value = keep + got[rank:]
                sent = [value] * len(masks)
            batch = [swap(data, mask) for data, mask in zip(sent, masks)]
            arrived += batch
            if index == 0 and not top_stage:
                stage_tables += call(
                    functools.partial(stage_table_kernel, lower_level, half),
                    [((2, 2, 3 * rank, rank), BF16)],
                    [upper] + batch[:2],
                    16 * unit,
                )
            if number == 0:
                if index == 0:
                    tables = call(
                        functools.partial(local_table_kernel, leaves),
                        [
                            turned,
                            rises,
                            ((2, 2, leaves * rank, (leaves + 1) * rank), BF16),
                            ((2, 2, leaves * rank, rank), BF16),
                            ((2, leaves * rank, rank), BF16),
                            ((4, rank, rank), F32),
                        ],
                        [local_operator, local_inverse] + list(u) + [v_operator, vt_inverse, up_inverse],
                        300 * unit,
                    )
                    vt[0], up[0], wide, down, feed, chip_feed = tables
                    chip_got = swap(chip_feed, 1)
                if last:
                    finished, norm = call(
                        last_value_kernel,
                        [(right_sides.shape, BF16), ((8, columns), F32)],
                        [base, u[0], down, mine, theirs] + norms,
                        100 * unit,
                    )
                    norm_got = swap(norm, 1)
                    base = call(
                        last_local_kernel,
                        [size],
                        [near, u[1], wide, coef, got, finished, current, feed, sibling_table]
                        + [mine, theirs],
                        100 * unit,
                    )[0]
                else:
                    args = [near, u[member], wide, coef, got]
                    base_list = list(base) if isinstance(base, (list, tuple)) else [base]
                    other_list = list(right) if member == 0 else [] if index == 0 else [current]
                    args += base_list + other_list
                    if index:
                        args += [u[other], down, feed, sibling_table, mine, theirs]
                    outs = [size]
                    if index:
                        outs.append(size if member == 0 else ((1, columns), F32))
                    counts = (len(base_list), len(other_list))
                    results = call(
                        functools.partial(local_kernel, member, index == 0, counts),
                        outs,
                        args,
                        200 * unit,
                    )
                    base = results[0]
                    coef, send, next_keep = call(
                        functools.partial(lift_kernel, other),
                        [coefs, lifted, message],
                        [base, vt[other], up[other]],
                        100 * unit,
                    )
                    next_got = swap(send, 1)
                    if index and member == 0:
                        current = results[1]
                    elif index:
                        norms.append(results[1])
            if not top_stage:
                extra = [norm, norm_got] if last and number == len(stages) - 2 else []
                shape = ((half + (8 if extra else 0), rank), F32)
                lift = stages[number + 1][0] - 1 if len(stages[number + 1]) > 1 else None
                results = call(
                    functools.partial(stage_kernel, member, half, lift),
                    [shape] * (1 if lift is None else 2),
                    [upper, stage_tables[number], value] + batch + extra,
                    8 * unit,
                )
                value, risen = results[0], results[-1]
        if index == 0:
            far_table, sibling_table = call(
                far_table_kernel,
                [
                    ((2, 2, (upper.shape[1] + 1) * rank, 2 * rank), BF16),
                    ((2, rank, rank), BF16),
                ],
                [upper, top_couplings, chip_feed, chip_got],
                100 * unit,
            )
        outs = [((8, columns), F32), message]
        if not last:
            outs = [message] * (3 if len(stages[0]) > 1 else 2)
        results = call(
            functools.partial(far_kernel, member, last, plan, half),
            outs,
            [upper, far_table] + ([keep, got] if last else [next_keep, next_got]) + arrived,
            20 * unit,
        )
        chip, chip_risen, mine = results[0], results[-2], results[-1]
        theirs = swap(mine, 1)
        if last:
            sums = chip + value[half:]
        else:
            keep, got = next_keep, next_got
        member = other
    solution = call(finish_kernel, [size], [u[1], down, base, mine, theirs], 30 * unit)[0]
    for number, stage in enumerate(stages[:-1]):
        masks = masks_of(number, stage)
        sums = sum([swap(sums, mask) for mask in masks], sums)
    return solution, sums[:STEPS]


def stages_of(levels_up):
    return [tuple(range(level, min(level + 2, levels_up))) for level in range(1, levels_up, 2)]


def solution(mesh):
    placed = (
        P(("rows", "leaf"), None),
        P(None, ("rows", "leaf"), None, None),
        P(None, ("rows", "leaf"), None, None, None),
        P(None, ("rows", "leaf"), None, None, None),
        P(None, ("rows", "leaf"), None, None, None, None),
        P(),
    )

    return jax.shard_map(
        body,
        mesh=mesh,
        in_specs=placed,
        out_specs=(P(("rows", "leaf"), None), P()),
        check_vma=False,
    )
```
